32 devices in a mesh: lon: 4 (over y, x), lat: 8 (over z, core).
Axes of the slice: x: 2, y: 2, z: 4, core: 2. Of those that a mesh axis runs over, the one named last changes fastest.
Arguments:
- tracer: float32 [1024, 64, 128], P('lon', 'lat'), may hold values from -6 to 6
- offsets: int32 [64], P('lat'), may hold values from 0 to 1023
- frac_lon: float32 [64], P('lat'), may hold values from 0 to 1
- frac_lat: float32 [64], P('lat'), may hold values from 0 to 1
- frac_lev: float32 [64], P('lat'), may hold values from 0 to 1
- metric: float32 [64], P('lat'), may hold values from 0.5 to 2
- vertical_coef: float32 [128], replicated, may hold values from 0.5 to 4
- inverses: float32 [64, 128, 128], P('lat'), may hold values from -0.1 to 0.6, as said below
Outputs:
- advected: float32 [1024, 64, 128], P('lon', 'lat')
- pressure: float32 [1024, 64, 128], P('lon', 'lat')
- residual: float32 [1024, 64, 128], P('lon', 'lat')
The draws below stay inside these ranges and needn't reach their ends.
Inputs may be any that keep to these rules, and one draw needn't show every extreme that they name: `inverses`: one matrix for each latitude row.
All inputs are finite; a program needn't handle non-finite values.
Results may differ from the reference program's by a relative error of at most 0.00016.
Values sent between devices are 32-bit elements; how exact they have to be, the bound alone decides.
A program may use at most 128 MiB of HBM per device.

```python
import math
import jax
import jax.numpy as jnp
from jax import lax

L = 128
ITERS = 3
NX = 1024
NY = 64


def draw_inverses(key, part):
    first_key, second_key = jax.random.split(jax.random.fold_in(key, 7))
    scales = jnp.exp(jax.random.uniform(first_key, (NY,), jnp.float32, jnp.log(0.1), jnp.log(0.5)))
    noise = jnp.clip(jax.random.normal(second_key, (NY, L, L), jnp.float32), -3.0, 3.0)
    identity = jnp.eye(L, dtype=jnp.float32)
    return scales[:, None, None] * (identity[None] + 0.03 * noise)


def set_ends(entries, rng, least, top_value):
    longest = entries.shape.index(max(entries.shape))
    spots = []
    for shift in (0, 1):
        where = [jax.random.randint(jax.random.fold_in(rng, axis), (), 0, length) for axis, length in enumerate(entries.shape)]
        where[longest] = (where[longest] + shift) % entries.shape[longest]
        spots.append(tuple(where))
    return entries.at[spots[0]].set(least).at[spots[1]].set(top_value)


def steps_of(own_key, extent, shards, least, largest):
    loudness = 1.0
    for dim, blocks in shards:
        draws = jax.random.uniform(jax.random.fold_in(jax.random.fold_in(own_key, 6), dim), (blocks,), jnp.float32, least / len(shards), largest / len(shards))
        loudness = loudness * jnp.repeat(jnp.exp(draws), extent[dim] // blocks).reshape((-1,) + (1,) * (len(extent) - 1 - dim))
    return loudness


def normal_values(rng, extent, spread, limit, cuts=(), held_as=jnp.bfloat16):
    entries = jax.random.normal(rng, extent, jnp.float32) * spread
    if len(cuts) > 0:
        entries = steps_of(rng, extent, cuts, -0.22, 0.18) * entries
    return jnp.clip(entries, min=-limit, max=limit).astype(held_as)


def setup_inputs(seed: int = 0) -> dict:
    arg_keys = jax.random.split(jax.random.key(seed), 9)
    tracer = normal_values(arg_keys[0], (NX, NY, L), 1.0, 6.0, ((0, 4), (1, 8)), jnp.float32)
    offsets = set_ends(jax.random.randint(arg_keys[1], (NY,), 0, NX), jax.random.fold_in(arg_keys[1], 1), 0, NX - 1).astype(jnp.int32)
    frac_lon = jnp.clip(1.0 * jax.random.uniform(arg_keys[2], (NY,), jnp.float32) ** steps_of(arg_keys[2], (NY,), ((0, 8),), -0.2, 0.2), 0.0, 1.0)
    frac_lat = jnp.clip(1.0 * jax.random.uniform(arg_keys[3], (NY,), jnp.float32) ** steps_of(arg_keys[3], (NY,), ((0, 8),), -0.2, 0.2), 0.0, 1.0)
    frac_lev = jnp.clip(1.0 * jax.random.uniform(arg_keys[4], (NY,), jnp.float32) ** steps_of(arg_keys[4], (NY,), ((0, 8),), -0.2, 0.2), 0.0, 1.0)
    metric = jnp.clip(jnp.exp(math.log(2.0) - 1.3862944 * jax.random.uniform(arg_keys[5], (NY,), jnp.float32) ** steps_of(arg_keys[5], (NY,), ((0, 8),), -0.2, 0.2)), 0.5, 2.0)
    vertical_coef = jnp.clip(jnp.exp(jax.random.uniform(arg_keys[6], (L,), jnp.float32, math.log(0.5), math.log(4.0))), 0.5, 4.0)
    inverses = draw_inverses(jax.random.fold_in(arg_keys[8], 71), 0)
    return {"tracer": tracer, "offsets": offsets, "frac_lon": frac_lon, "frac_lat": frac_lat, "frac_lev": frac_lev, "metric": metric, "vertical_coef": vertical_coef, "inverses": inverses}


def cubic_weights(fraction):
    return (-fraction * (fraction - 1.0) * (fraction - 2.0) / 6.0,
            (fraction + 1.0) * (fraction - 1.0) * (fraction - 2.0) / 2.0,
            -(fraction + 1.0) * fraction * (fraction - 2.0) / 2.0,
            (fraction + 1.0) * fraction * (fraction - 1.0) / 6.0)


def operate(field, metric, vertical_coef):
    eastern = jnp.roll(field, -1, 0)
    western = jnp.roll(field, 1, 0)
    padded = jnp.pad(field, ((0, 0), (1, 1), (0, 0)))
    levels = jnp.pad(field, ((0, 0), (0, 0), (1, 1)))
    result = metric[None, :, None] * (2.0 * field - eastern - western)
    result = result + (2.0 * field - padded[:, 2:] - padded[:, :-2])
    result = result + vertical_coef[None, None, :] * (2.0 * field - levels[:, :, 2:] - levels[:, :, :-2])
    return result + 0.1 * field


def precondition(inverses, field):
    return jnp.einsum('jkm,xjm->xjk', inverses, field, precision=lax.Precision.HIGHEST)


def reference(tracer, offsets, frac_lon, frac_lat, frac_lev, metric, vertical_coef, inverses):
    lat_weights = cubic_weights(frac_lat)
    padded = jnp.pad(tracer, ((0, 0), (1, 2), (0, 0)))
    lat_mixed = jnp.zeros_like(tracer)
    for tap_index in range(4):
        lat_mixed = lat_mixed + lat_weights[tap_index][None, :, None] * padded[:, tap_index:tap_index + NY]
    lev_weights = cubic_weights(frac_lev)
    padded = jnp.pad(lat_mixed, ((0, 0), (0, 0), (1, 2)))
    lev_mixed = jnp.zeros_like(tracer)
    for tap_index in range(4):
        lev_mixed = lev_mixed + lev_weights[tap_index][None, :, None] * padded[:, :, tap_index:tap_index + L]
    lon_weights = cubic_weights(frac_lon)
    columns = jnp.arange(NX, dtype=jnp.int32)[:, None]
    row_index = jnp.arange(NY, dtype=jnp.int32)[None, :]
    advected = jnp.zeros_like(tracer)
    for tap_index in range(4):
        source = jnp.mod(columns - offsets.astype(jnp.int32)[None, :] + (tap_index - 1), NX).astype(jnp.int32)
        advected = advected + lon_weights[tap_index][None, :, None] * lev_mixed[source, row_index]
    pressure = jnp.zeros_like(advected)
    residual = advected
    first = precondition(inverses, residual)
    directions = [first]
    images = [operate(first, metric, vertical_coef)]
    along = jnp.sum(residual * images[0])
    squares = [jnp.sum(images[0] * images[0])]
    for step in range(ITERS):
        alpha = along / squares[step]
        pressure = pressure + alpha * directions[step]
        residual = residual - alpha * images[step]
        if step + 1 < ITERS:
            search = precondition(inverses, residual)
            image_new = operate(search, metric, vertical_coef)
            direction_new = search
            for prior in range(step + 1):
                factor = -jnp.sum(image_new * images[prior]) / squares[prior]
                direction_new = direction_new + factor * directions[prior]
                image_new = image_new + factor * images[prior]
            directions.append(direction_new)
            images.append(image_new)
            along = jnp.sum(residual * image_new)
            squares.append(jnp.sum(image_new * image_new))
    return advected, pressure, residual
```

```python
import functools

import jax
import jax.numpy as jnp
from jax import lax
from jax.experimental import pallas as pl
from jax.experimental.pallas import tpu as pltpu
from jax.sharding import PartitionSpec as P

ITERS = 3
DEEP = ITERS
PAD = 8
VM = pl.BlockSpec(memory_space=pltpu.VMEM)
SM = pl.BlockSpec(memory_space=pltpu.SMEM)
ANY = pl.BlockSpec(memory_space=pl.ANY)
F32 = jnp.float32
BF16 = jnp.bfloat16
MESH = pl.DeviceIdType.MESH


def cubic_weights(f):
    return (
        -f * (f - 1.0) * (f - 2.0) * (1.0 / 6.0),
        (f + 1.0) * (f - 1.0) * (f - 2.0) * 0.5,
        -(f + 1.0) * f * (f - 2.0) * 0.5,
        (f + 1.0) * f * (f - 1.0) * (1.0 / 6.0),
    )


def shape(*dims, dtype=F32):
    return jax.ShapeDtypeStruct(dims, dtype)


def signal(sem, peer):
    pl.semaphore_signal(sem, inc=1, device_id=peer, device_id_type=MESH)


def remote(src, dst, send_sem, recv_sem, peer):
    return pltpu.make_async_remote_copy(
        src_ref=src,
        dst_ref=dst,
        send_sem=send_sem,
        recv_sem=recv_sem,
        device_id=peer,
        device_id_type=MESH,
    )


def split(x):
    high = x.astype(BF16)
    return high, (x - high.astype(F32)).astype(BF16)


def pieces(first, last, size):
    out = []
    while first < last:
        step = size if last - first < 2 * size else size
        step = min(step, last - first)
        out.append((first, step))
        first += step
    return out


def fold(x):
    return jnp.sum(x.reshape(x.shape[0] // 8, 8, x.shape[1]), axis=0)


def coefficients(t):
    right = t[:3]
    gram = [[t[3], t[4], t[5]], [t[4], t[6], t[7]], [t[5], t[7], t[8]]]
    zero = jnp.zeros_like(t[0])

    def form(p, q):
        total = zero
        for k in range(3):
            for l in range(3):
                if p[k] is not None and q[l] is not None:
                    total = total + p[k] * q[l] * gram[k][l]
        return total

    def add(p, s, q):
        return [x if y is None else (s * y if x is None else x + s * y) for x, y in zip(p, q)]

    q = [[zero + 1.0, None, None]]
    rho, pi = [None] * 3, [None] * 3
    squares = [form(q[0], q[0])]
    for i in range(ITERS):
        along = form(q[i], rho)
        for k in range(3):
            if q[i][k] is not None:
                along = along + q[i][k] * right[k]
        alpha = along / squares[i]
        pi = add(pi, alpha, q[i])
        rho = add(rho, -alpha, q[i])
        if i + 1 < ITERS:
            z = [zero + 1.0, rho[0], rho[1]]
            new = z
            for l in range(i + 1):
                new = add(new, -form(z, q[l]) / squares[l], q[l])
            q.append(new)
            squares.append(form(new, new))
    return rho, pi


def step_kernel(lons, lats, off, f_lon, f_lat, f_lev, metric, vc_ref, tracer, inv, *refs):
    (r_ext, v0, v1, v2, w0, w1, w2, tot) = refs[:8]
    (t, double, s_buf, v_buf, g_buf, f_buf, inv_ext, met, packed, lhs, part, every) = refs[8:20]
    (t_sem, i_sem, hs, hr, ns, nr, p1s, p1r, p2s, p2r, ws, wr, es, er, fs, fr, rs, rr) = refs[20:]
    width, rows, levels = tracer.shape
    quarter = width // lons
    deep = DEEP
    ext, wide = rows + 2 * deep, width + 2 * PAD
    me, lat = lax.axis_index("lon"), lax.axis_index("lat")
    ring = lambda k: lax.rem(me + (k + lons), lons)
    has_low, has_high = lat > 0, lat < lats - 1
    below = {"lat": lax.max(lat - 1, 0)}
    above = {"lat": lax.min(lat + 1, lats - 1)}
    devices = lons * lats
    mine = me * lats + lat
    lane = lax.broadcasted_iota(jnp.int32, (1, levels), 1)

    def peer_of(k):
        index = lax.rem(mine + k, devices)
        return {"lon": lax.div(index, lats), "lat": lax.rem(index, lats)}

    first_rows = [rows - 1, 0, 1] + list(range(2, rows - 1))
    loads = {j: pltpu.make_async_copy(tracer.at[:, j, :], t.at[j + 1], t_sem.at[j]) for j in range(rows)}
    for j in first_rows:
        loads[j].start()
    matrices = pltpu.make_async_copy(inv, inv_ext.at[pl.ds(deep, rows)], i_sem)
    matrices.start()

    barrier = pltpu.get_barrier_semaphore()
    lax.fori_loop(1, devices, lambda k, c: (signal(barrier, peer_of(k)), c)[1], 0)

    for j in range(rows):
        met[deep + j : deep + j + 1, :] = jnp.full((1, levels), metric[j], F32)
        f_buf[j, :PAD, :] = jnp.zeros((PAD, levels), F32)
        f_buf[j, wide + PAD :, :] = jnp.zeros((PAD, levels), F32)
    for w in (w0, w1, w2):
        for e in range(w.shape[0]):
            w[e, :PAD, :] = jnp.zeros((PAD, levels), F32)
            w[e, wide + PAD :, :] = jnp.zeros((PAD, levels), F32)

    def clear(ref, first, count):
        ref[first : first + count] = jnp.zeros((count,) + ref.shape[1:], F32)

    @pl.when(jnp.logical_not(has_low))
    def _():
        clear(t, 0, 1)
        clear(r_ext, 0, deep)
        clear(inv_ext, 0, deep)
        met[:deep, :] = jnp.zeros((deep, levels), F32)

    @pl.when(jnp.logical_not(has_high))
    def _():
        clear(t, rows + 1, 2)
        clear(r_ext, deep + rows, deep)
        clear(inv_ext, deep + rows, deep)
        met[deep + rows : ext, :] = jnp.zeros((deep, levels), F32)

    up_row = remote(t.at[rows], t.at[0], hs.at[0], hr.at[0], above)
    down_rows = remote(t.at[pl.ds(1, 2)], t.at[pl.ds(rows + 1, 2)], hs.at[1], hr.at[1], below)
    up_inv = remote(inv_ext.at[pl.ds(rows, deep)], inv_ext.at[pl.ds(0, deep)], hs.at[2], hr.at[2], above)
    down_inv = remote(
        inv_ext.at[pl.ds(deep, deep)], inv_ext.at[pl.ds(deep + rows, deep)], hs.at[3], hr.at[3], below
    )
    up_met = [remote(met.at[rows + m], met.at[m], ns.at[m], nr.at[m], above) for m in range(deep)]
    down_met = [
        remote(met.at[deep + m], met.at[deep + rows + m], ns.at[deep + m], nr.at[deep + m], below)
        for m in range(deep)
    ]
    for j in first_rows[:3]:
        loads[j].wait()
    pl.semaphore_wait(barrier, devices - 1)

    @pl.when(has_high)
    def _():
        up_row.start()

    @pl.when(has_low)
    def _():
        down_rows.start()

    for j in first_rows[3:]:
        loads[j].wait()

    def mix(j):
        a = cubic_weights(f_lat[j])
        b = cubic_weights(f_lev[j])
        taps = {m: jnp.where((lane + m >= 0) & (lane + m < levels), b[m + 1], 0.0) for m in (-1, 1, 2)}
        buffer = double.at[j % 2]
        for first, size in pieces(0, width, 64):
            at = pl.ds(first, size)
            x = a[0] * t[j, at, :] + a[1] * t[j + 1, at, :] + a[2] * t[j + 2, at, :] + a[3] * t[j + 3, at, :]
            total = b[1] * x
            for m in (-1, 1, 2):
                total = total + taps[m] * pltpu.roll(x, (-m) % levels, 1)
            buffer[at, :] = total
            buffer[pl.ds(width + first, size), :] = total
        start = width - lax.rem(off[j], width)
        for first, size in pieces(0, width, 64):
            s_buf[j, pl.ds(first, size), :] = buffer[pl.ds(start + first, size), :]

    def part_of(device, j):
        return pl.multiple_of(lax.rem(device + j, lons) * quarter, quarter)

    def all_of(ref, j, count, send_sem, recv_sem):
        return remote(ref.at[j, pl.ds(0, count)], ref.at[j, pl.ds(0, count)], send_sem, recv_sem, {"lon": ring(1)})

    def spread(j):
        for k in range(1, lons):
            q = ring(k)
            remote(
                s_buf.at[j, pl.ds(part_of(q, j), quarter)], v_buf.at[j, me], p1s.at[j], p1r.at[j], {"lon": q}
            ).start()
        v_buf[j, me] = s_buf[j, pl.ds(part_of(me, j), quarter), :]

    def deliver(j):
        all_of(v_buf, j, lons - 1, p1s.at[j], p1r.at[j]).wait_recv()
        offset = off[j]
        rest = lax.rem(offset, width)
        block = lax.rem(lax.div(offset, width), lons)
        begin = part_of(me, j)
        some = min(32, quarter)
        for first, size in pieces(0, quarter, some):
            place = lax.broadcasted_iota(jnp.int32, (size, levels), 0) + (begin + first)
            turn = jnp.where(place < rest, lax.rem(block + 1, lons), block)
            x = [v_buf[j, s, pl.ds(first, size), :] for s in range(lons)]
            bit = lons // 2
            while bit:
                mask = (turn & bit) != 0
                x = [jnp.where(mask, x[(d - bit) % lons], x[d]) for d in range(lons)]
                bit //= 2
            for d in range(lons):
                g_buf[j, d, pl.ds(first, size), :] = x[d]
        here = pl.ds(pl.multiple_of(2 * PAD + begin, PAD), quarter)
        west = pl.ds(PAD, PAD)
        east = pl.ds(2 * PAD + width, PAD)
        for k in range(1, lons):
            d = ring(k)
            remote(g_buf.at[j, d], f_buf.at[j, here], p2s.at[j], p2r.at[j], {"lon": d}).start()
        f_buf[j, here, :] = g_buf[j, me]
        part = lax.rem(me + j, lons)

        @pl.when(part == lons - 1)
        def _():
            for k in range(1, lons):
                src = g_buf.at[j, ring(k - 1), pl.ds(quarter - PAD, PAD)]
                remote(src, f_buf.at[j, west], ws.at[j], wr.at[j], {"lon": ring(k)}).start()
            f_buf[j, west, :] = g_buf[j, ring(-1), quarter - PAD :, :]

        @pl.when(part == 0)
        def _():
            for k in range(1, lons):
                src = g_buf.at[j, ring(k + 1), pl.ds(0, PAD)]
                remote(src, f_buf.at[j, east], es.at[j], er.at[j], {"lon": ring(k)}).start()
            f_buf[j, east, :] = g_buf[j, ring(1), :PAD, :]

    def edge_wait(j, send_sem, recv_sem, owner, count):
        block = f_buf.at[j, pl.ds(PAD, PAD * count)]
        return remote(block, block, send_sem, recv_sem, {"lon": ring(1)})

    def arrive(j):
        main = f_buf.at[j, pl.ds(2 * PAD, (lons - 1) * quarter)]
        remote(main, main, p2s.at[j], p2r.at[j], {"lon": ring(1)}).wait_recv()
        part = lax.rem(me + j, lons)

        @pl.when(part != lons - 1)
        def _():
            edge_wait(j, ws.at[j], wr.at[j], lons - 1, 1).wait_recv()

        @pl.when(part != 0)
        def _():
            edge_wait(j, es.at[j], er.at[j], 0, 1).wait_recv()

        c = cubic_weights(f_lon[j])
        for first, size in pieces(0, wide, 64):
            r_ext[deep + j, pl.ds(first, size), :] = sum(
                c[m] * f_buf[j, pl.ds(first + PAD - 1 + m, size), :] for m in range(4)
            )
        if j < deep:
            @pl.when(has_low)
            def _():
                low_copy(j).start()
        if j >= rows - deep:
            @pl.when(has_high)
            def _():
                high_copy(j).start()

    def low_copy(j):
        return remote(r_ext.at[deep + j], r_ext.at[deep + rows + j], fs.at[j], fr.at[j], below)

    def high_copy(j):
        m = j - (rows - deep)
        return remote(r_ext.at[deep + j], r_ext.at[m], fs.at[deep + m], fr.at[deep + m], above)

    def settle(j):
        all_of(g_buf, j, lons - 1, p2s.at[j], p2r.at[j]).wait_send()
        all_of(v_buf, j, lons - 1, p1s.at[j], p1r.at[j]).wait_send()
        part = lax.rem(me + j, lons)

        @pl.when(part == lons - 1)
        def _():
            edge_wait(j, ws.at[j], wr.at[j], lons - 1, lons - 1).wait_send()

        @pl.when(part == 0)
        def _():
            edge_wait(j, es.at[j], er.at[j], 0, lons - 1).wait_send()

    vc = vc_ref[...]
    up = jnp.where(lane < levels - 1, vc, 0.0)
    down = jnp.where(lane > 0, vc, 0.0)
    ws_refs, vs_refs = (w0, w1, w2), (v0, v1, v2)
    acc = [jnp.zeros((8, levels), F32) for _ in range(9)]

    def pack(e):
        high, low = split(inv_ext[e])
        packed[e, :levels, :levels] = high
        packed[e, :levels, levels:] = high
        packed[e, levels:, :levels] = low
        packed[e, levels:, levels:] = jnp.zeros((levels, levels), BF16)

    def solve(k, e, slot):
        both = lax.dot_general(
            lhs[slot], packed[e], (((1,), (1,)), ((), ())), preferred_element_type=F32
        )
        ws_refs[k][e - k, pl.ds(PAD, wide), :] = both[:, :levels] + both[:, levels:]

    def load_lhs(slot, first, size, v):
        high, low = split(v)
        lhs[slot, pl.ds(first, size), :levels] = high
        lhs[slot, pl.ds(first, size), levels:] = low

    def begin(e, slot):
        for first, size in pieces(0, wide, 64):
            load_lhs(slot, first, size, r_ext[e, pl.ds(first, size), :])
        solve(0, e, slot)

    def stencil(k, e, first, size):
        w = ws_refs[k]
        n = e - k
        m = met[e : e + 1, :]
        centre = w[n, pl.ds(first + PAD, size), :]
        result = (2.0 * m + 2.1 + 2.0 * vc) * centre
        result = result - m * (
            w[n, pl.ds(first + PAD + 1, size), :] + w[n, pl.ds(first + PAD - 1, size), :]
        )
        result = result - (w[n - 1, pl.ds(first + PAD, size), :] + w[n + 1, pl.ds(first + PAD, size), :])
        result = result - up * pltpu.roll(centre, levels - 1, 1)
        return result - down * pltpu.roll(centre, 1, 1)

    pairs = {0: ((0, "r", 0), (3, 0, 0)), 1: ((1, "r", 1), (4, 0, 1), (6, 1, 1)),
             2: ((2, "r", 2), (5, 0, 2), (7, 1, 2), (8, 2, 2))}

    def apply(k, e, slot):
        inside = deep <= e < deep + rows
        if k + 1 < ITERS:
            for first, size in pieces(0, wide, 64):
                v = stencil(k, e, first, size)
                load_lhs(slot, first, size, v)
                if inside:
                    vs_refs[k][e - deep, pl.ds(first, size), :] = v
            solve(k + 1, e, slot)
            if inside:
                for first, size in pieces(PAD, PAD + width, 64):
                    gather(k, e, first, size, vs_refs[k][e - deep, pl.ds(first, size), :])
        else:
            for first, size in pieces(PAD, PAD + width, 64):
                v = stencil(k, e, first, size)
                vs_refs[k][e - deep, pl.ds(first, size), :] = v
                gather(k, e, first, size, v)

    def gather(k, e, first, size, v):
        for n, p, q in pairs[k]:
            if p == "r":
                other = r_ext[e, pl.ds(first, size), :]
            elif p == k:
                other = v
            else:
                other = vs_refs[p][e - deep, pl.ds(first, size), :]
            acc[n] = acc[n] + fold(other * v)

    plain = lambda j: 1 <= j <= rows - 3
    edges = [j for j in range(rows) if j < deep or j >= rows - deep]
    order = [j for j in edges if plain(j)] + [j for j in edges if not plain(j)]
    order += [j for j in range(rows) if j not in order]
    waited = False
    sent_inv = False
    for j in order:
        if not plain(j) and not waited:
            waited = True

            @pl.when(has_low)
            def _():
                up_row.wait_recv()

            @pl.when(has_high)
            def _():
                down_rows.wait_recv()

        mix(j)
        spread(j)
        if not sent_inv:
            sent_inv = True
            matrices.wait()

            @pl.when(has_high)
            def _():
                up_inv.start()
                for copy in up_met:
                    copy.start()

            @pl.when(has_low)
            def _():
                down_inv.start()
                for copy in down_met:
                    copy.start()

    for e in range(deep, deep + rows):
        pack(e)
    for j in order:
        deliver(j)

    @pl.when(has_low)
    def _():
        up_inv.wait_recv()
        for copy in up_met:
            copy.wait_recv()

    @pl.when(has_high)
    def _():
        down_inv.wait_recv()
        for copy in down_met:
            copy.wait_recv()

    for e in list(range(deep)) + list(range(deep + rows, ext)):
        pack(e)

    done = {}
    slots = [0]

    def slot():
        slots[0] += 1
        return slots[0] % 2

    def ready():
        again = True
        while again:
            again = False
            for k in range(ITERS):
                for e in range(k + 1, ext - k - 1):
                    if ("v", k, e) not in done and all(("w", k, e + m) in done for m in (-1, 0, 1)):
                        apply(k, e, slot())
                        done["v", k, e] = True
                        if k + 1 < ITERS:
                            done["w", k + 1, e] = True
                        again = True

    def first_solve(e):
        begin(e, slot())
        done["w", 0, e] = True

    held = order[len(edges) :]
    for j in order[: len(edges)]:
        arrive(j)
    for j in order[: len(edges)]:
        first_solve(deep + j)
    ready()
    for j in held:
        arrive(j)
        first_solve(deep + j)
    ready()

    @pl.when(has_low)
    def _():
        for m in range(deep):
            high_copy(rows - deep + m).wait_recv()

    @pl.when(has_high)
    def _():
        for m in range(deep):
            low_copy(m).wait_recv()

    for e in list(range(deep)) + list(range(deep + rows, ext)):
        first_solve(e)
    ready()

    row = jnp.zeros((1, levels), F32)
    for n in range(9):
        row = jnp.where(lane == n, jnp.sum(jnp.sum(acc[n], axis=0, keepdims=True), axis=1, keepdims=True), row)
    part[...] = row
    every[mine] = row

    def tell(k, carry):
        remote(part, every.at[mine], rs, rr, peer_of(k)).start()
        return carry

    lax.fori_loop(1, devices, tell, 0)
    for j in range(rows):
        settle(j)

    @pl.when(has_high)
    def _():
        up_row.wait_send()
        up_inv.wait_send()
        for copy in up_met:
            copy.wait_send()
        for m in range(deep):
            high_copy(rows - deep + m).wait_send()

    @pl.when(has_low)
    def _():
        down_rows.wait_send()
        down_inv.wait_send()
        for copy in down_met:
            copy.wait_send()
        for m in range(deep):
            low_copy(m).wait_send()

    others = every.at[pl.ds(0, devices - 1)]
    totals = remote(others, others, rs, rr, {"lon": ring(1)})
    totals.wait_recv()
    totals.wait_send()
    tot[...] = jnp.broadcast_to(jnp.sum(every[...], axis=0), tot.shape)


def final_kernel(tot, r_ext, v0, v1, v2, w0, w1, w2, a_out, p_out, r_out, a_buf, p_buf, r_buf, sem):
    rows = v0.shape[0]
    levels = v0.shape[2]
    width = v0.shape[1] - 2 * PAD
    deep = DEEP
    total = tot[0:1, :]
    size = min(32, width)
    copies = []

    def ship(buf, out, c, n):
        at = pl.ds(c * size * rows, size * rows)
        copy = pltpu.make_async_copy(buf.at[at], out.at[at], sem.at[n, c])
        copy.start()
        copies.append(copy)

    for c in range(width // size):
        for j in range(rows):
            a_buf[pl.ds(c * size * rows + j, size, stride=rows), :] = r_ext[
                deep + j, pl.ds(PAD + c * size, size), :
            ]
        ship(a_buf, a_out, c, 0)
    rho, pi = coefficients([total[:, n : n + 1] for n in range(9)])
    rho = [jnp.broadcast_to(x, (8, levels))[0:1] for x in rho]
    pi = [jnp.broadcast_to(x, (8, levels))[0:1] for x in pi]
    for c in range(width // size):
        for j in range(rows):
            where = pl.ds(c * size * rows + j, size, stride=rows)
            at = pl.ds(PAD + c * size, size)
            wat = pl.ds(2 * PAD + c * size, size)
            p_buf[where, :] = (
                pi[0] * w0[deep + j, wat, :] + pi[1] * w1[deep - 1 + j, wat, :] + pi[2] * w2[deep - 2 + j, wat, :]
            )
            r_buf[where, :] = r_ext[deep + j, at, :] + (
                rho[0] * v0[j, at, :] + rho[1] * v1[j, at, :] + rho[2] * v2[j, at, :]
            )
        ship(p_buf, p_out, c, 1)
        ship(r_buf, r_out, c, 2)
    for copy in copies:
        copy.wait()


def body(tracer, offsets, frac_lon, frac_lat, frac_lev, metric, vertical_coef, inverses):
    width, rows, levels = tracer.shape
    lons, lats = lax.axis_size("lon"), lax.axis_size("lat")
    deep = DEEP
    ext, wide, quarter = rows + 2 * deep, width + 2 * PAD, width // lons
    devices = lons * lats
    dma = pltpu.SemaphoreType.DMA
    field = [shape(rows, wide, levels)] * 3
    sides = [shape(ext - 2 * k, wide + 2 * PAD, levels) for k in range(3)]
    r_ext, v0, v1, v2, w0, w1, w2, tot = pl.pallas_call(
        functools.partial(step_kernel, lons, lats),
        out_shape=[shape(ext, wide, levels)] + field + sides + [shape(8, levels)],
        in_specs=[SM] * 5 + [VM, ANY, ANY],
        out_specs=[VM] * 8,
        scratch_shapes=[
            pltpu.VMEM((rows + 3, width, levels), F32),
            pltpu.VMEM((2, 2 * width, levels), F32),
            pltpu.VMEM((rows, width, levels), F32),
            pltpu.VMEM((rows, lons, quarter, levels), F32),
            pltpu.VMEM((rows, lons, quarter, levels), F32),
            pltpu.VMEM((rows, wide + 2 * PAD, levels), F32),
            pltpu.VMEM((ext, levels, levels), F32),
            pltpu.VMEM((ext, levels), F32),
            pltpu.VMEM((ext, 2 * levels, 2 * levels), BF16),
            pltpu.VMEM((2, wide, 2 * levels), BF16),
            pltpu.VMEM((1, levels), F32),
            pltpu.VMEM((devices, 1, levels), F32),
            dma((rows,)),
            dma,
            dma((4,)),
            dma((4,)),
            dma((2 * deep,)),
            dma((2 * deep,)),
        ]
        + [dma((rows,))] * 8
        + [dma((2 * deep,))] * 2
        + [dma] * 2,
        compiler_params=pltpu.CompilerParams(
            collective_id=1, has_side_effects=True, vmem_limit_bytes=30 * 2**20
        ),
    )(offsets, frac_lon, frac_lat, frac_lev, metric, vertical_coef.reshape(1, levels), tracer, inverses)
    whole = shape(width * rows, levels)
    buffer = pltpu.VMEM((width * rows, levels), F32)
    outs = pl.pallas_call(
        final_kernel,
        out_shape=[whole] * 3,
        in_specs=[VM] * 8,
        out_specs=[ANY] * 3,
        scratch_shapes=[buffer] * 3 + [dma((3, width // min(32, width)))],
        compiler_params=pltpu.CompilerParams(vmem_limit_bytes=20 * 2**20),
    )(tot, r_ext, v0, v1, v2, w0, w1, w2)
    return tuple(x.reshape(width, rows, levels) for x in outs)


def solution(mesh):
    cube = P("lon", "lat", None)
    in_specs = (cube, P("lat"), P("lat"), P("lat"), P("lat"), P("lat"), P(), P("lat", None, None))
    return jax.shard_map(
        body, mesh=mesh, in_specs=in_specs, out_specs=(cube, cube, cube), check_vma=False
    )
```

```python
import functools

import jax
import jax.numpy as jnp
from jax import lax
from jax.experimental import pallas as pl
from jax.experimental.pallas import tpu as pltpu
from jax.sharding import PartitionSpec as P

ITERS = 3
DEEP = ITERS
PAD = 8
VM = pl.BlockSpec(memory_space=pltpu.VMEM)
ANY = pl.BlockSpec(memory_space=pl.ANY)
HBM = pl.BlockSpec(memory_space=pltpu.HBM)
F32 = jnp.float32
BF16 = jnp.bfloat16
MESH = pl.DeviceIdType.MESH


def cubic_weights(f):
    return (
        -f * (f - 1.0) * (f - 2.0) * (1.0 / 6.0),
        (f + 1.0) * (f - 1.0) * (f - 2.0) * 0.5,
        -(f + 1.0) * f * (f - 2.0) * 0.5,
        (f + 1.0) * f * (f - 1.0) * (1.0 / 6.0),
    )


def shape(*dims, dtype=F32):
    return jax.ShapeDtypeStruct(dims, dtype)


def signal(sem, peer):
    pl.semaphore_signal(sem, inc=1, device_id=peer, device_id_type=MESH)


def remote(src, dst, send_sem, recv_sem, peer):
    return pltpu.make_async_remote_copy(
        src_ref=src,
        dst_ref=dst,
        send_sem=send_sem,
        recv_sem=recv_sem,
        device_id=peer,
        device_id_type=MESH,
    )


def split(x):
    high = x.astype(BF16)
    return high, (x - high.astype(F32)).astype(BF16)


def pieces(first, last, size):
    out = []
    while first < last:
        step = size if last - first < 2 * size else size
        step = min(step, last - first)
        out.append((first, step))
        first += step
    return out


def fold(x):
    return jnp.sum(x.reshape(x.shape[0] // 8, 8, x.shape[1]), axis=0)


def coefficients(t):
    right = t[:3]
    gram = [[t[3], t[4], t[5]], [t[4], t[6], t[7]], [t[5], t[7], t[8]]]
    zero = jnp.zeros_like(t[0])

    def form(p, q):
        total = zero
        for k in range(3):
            for l in range(3):
                if p[k] is not None and q[l] is not None:
                    total = total + p[k] * q[l] * gram[k][l]
        return total

    def add(p, s, q):
        return [x if y is None else (s * y if x is None else x + s * y) for x, y in zip(p, q)]

    q = [[zero + 1.0, None, None]]
    rho, pi = [None] * 3, [None] * 3
    squares = [form(q[0], q[0])]
    for i in range(ITERS):
        along = form(q[i], rho)
        for k in range(3):
            if q[i][k] is not None:
                along = along + q[i][k] * right[k]
        alpha = along / squares[i]
        pi = add(pi, alpha, q[i])
        rho = add(rho, -alpha, q[i])
        if i + 1 < ITERS:
            z = [zero + 1.0, rho[0], rho[1]]
            new = z
            for l in range(i + 1):
                new = add(new, -form(z, q[l]) / squares[l], q[l])
            q.append(new)
            squares.append(form(new, new))
    return rho, pi


def step_kernel(lons, lats, *refs):
    scalars, (tracer, inv), refs = refs[:6], refs[6:8], refs[8:]
    (r_ext, v0, v1, v2, w0, w1, w2, tot) = refs[:8]
    (t, double, s_buf, v_buf, g_buf, f_buf, inv_ext, met, packed, lhs, part, every) = refs[8:20]
    (off, f_lon, f_lat, f_lev, metric, vc_ref, c_sem), refs = refs[20:27], refs[:20] + refs[27:]
    (t_sem, i_sem, hs, hr, ns, nr, p1s, p1r, p2s, p2r, ws, wr, es, er, fs, fr, rs, rr) = refs[20:]
    width, rows, levels = tracer.shape
    quarter = width // lons
    deep = DEEP
    ext, wide = rows + 2 * deep, width + 2 * PAD
    me, lat = lax.axis_index("lon"), lax.axis_index("lat")
    ring = lambda k: lax.rem(me + (k + lons), lons)
    has_low, has_high = lat > 0, lat < lats - 1
    below = {"lat": lax.max(lat - 1, 0)}
    above = {"lat": lax.min(lat + 1, lats - 1)}
    devices = lons * lats
    mine = me * lats + lat
    lane = lax.broadcasted_iota(jnp.int32, (1, levels), 1)

    def peer_of(k):
        index = lax.rem(mine + k, devices)
        return {"lon": lax.div(index, lats), "lat": lax.rem(index, lats)}

    first_rows = [rows - 1, 0, 1] + list(range(2, rows - 1))
    loads = {j: pltpu.make_async_copy(tracer.at[:, j, :], t.at[j + 1], t_sem.at[j]) for j in range(rows)}
    for j in first_rows:
        loads[j].start()
    fetches = [
        pltpu.make_async_copy(src, dst, c_sem.at[n])
        for n, (src, dst) in enumerate(zip(scalars, (off, f_lon, f_lat, f_lev, metric, vc_ref)))
    ]
    for copy in fetches:
        copy.start()
    matrices = pltpu.make_async_copy(inv, inv_ext.at[pl.ds(deep, rows)], i_sem)
    matrices.start()

    barrier = pltpu.get_barrier_semaphore()
    lax.fori_loop(1, devices, lambda k, c: (signal(barrier, peer_of(k)), c)[1], 0)

    for copy in fetches:
        copy.wait()
    for j in range(rows):
        met[deep + j : deep + j + 1, :] = jnp.full((1, levels), metric[j], F32)
        f_buf[j, :PAD, :] = jnp.zeros((PAD, levels), F32)
        f_buf[j, wide + PAD :, :] = jnp.zeros((PAD, levels), F32)
    for w in (w0, w1, w2):
        for e in range(w.shape[0]):
            w[e, :PAD, :] = jnp.zeros((PAD, levels), F32)
            w[e, wide + PAD :, :] = jnp.zeros((PAD, levels), F32)

    def clear(ref, first, count):
        ref[first : first + count] = jnp.zeros((count,) + ref.shape[1:], F32)

    @pl.when(jnp.logical_not(has_low))
    def _():
        clear(t, 0, 1)
        clear(r_ext, 0, deep)
        clear(inv_ext, 0, deep)
        met[:deep, :] = jnp.zeros((deep, levels), F32)

    @pl.when(jnp.logical_not(has_high))
    def _():
        clear(t, rows + 1, 2)
        clear(r_ext, deep + rows, deep)
        clear(inv_ext, deep + rows, deep)
        met[deep + rows : ext, :] = jnp.zeros((deep, levels), F32)

    up_row = remote(t.at[rows], t.at[0], hs.at[0], hr.at[0], above)
    down_rows = remote(t.at[pl.ds(1, 2)], t.at[pl.ds(rows + 1, 2)], hs.at[1], hr.at[1], below)
    up_inv = remote(inv_ext.at[pl.ds(rows, deep)], inv_ext.at[pl.ds(0, deep)], hs.at[2], hr.at[2], above)
    down_inv = remote(
        inv_ext.at[pl.ds(deep, deep)], inv_ext.at[pl.ds(deep + rows, deep)], hs.at[3], hr.at[3], below
    )
    up_met = [remote(met.at[rows + m], met.at[m], ns.at[m], nr.at[m], above) for m in range(deep)]
    down_met = [
        remote(met.at[deep + m], met.at[deep + rows + m], ns.at[deep + m], nr.at[deep + m], below)
        for m in range(deep)
    ]
    for j in first_rows[:3]:
        loads[j].wait()
    pl.semaphore_wait(barrier, devices - 1)

    @pl.when(has_high)
    def _():
        up_row.start()

    @pl.when(has_low)
    def _():
        down_rows.start()

    for j in first_rows[3:]:
        loads[j].wait()

    def mix(j):
        a = cubic_weights(f_lat[j])
        b = cubic_weights(f_lev[j])
        taps = {m: jnp.where((lane + m >= 0) & (lane + m < levels), b[m + 1], 0.0) for m in (-1, 1, 2)}
        buffer = double.at[j % 2]
        for first, size in pieces(0, width, 64):
            at = pl.ds(first, size)
            x = a[0] * t[j, at, :] + a[1] * t[j + 1, at, :] + a[2] * t[j + 2, at, :] + a[3] * t[j + 3, at, :]
            total = b[1] * x
            for m in (-1, 1, 2):
                total = total + taps[m] * pltpu.roll(x, (-m) % levels, 1)
            buffer[at, :] = total
            buffer[pl.ds(width + first, size), :] = total
        start = width - lax.rem(off[j], width)
        for first, size in pieces(0, width, 64):
            s_buf[j, pl.ds(first, size), :] = buffer[pl.ds(start + first, size), :]

    def part_of(device, j):
        return pl.multiple_of(lax.rem(device + j, lons) * quarter, quarter)

    def all_of(ref, j, count, send_sem, recv_sem):
        return remote(ref.at[j, pl.ds(0, count)], ref.at[j, pl.ds(0, count)], send_sem, recv_sem, {"lon": ring(1)})

    def spread(j):
        for k in range(1, lons):
            q = ring(k)
            remote(
                s_buf.at[j, pl.ds(part_of(q, j), quarter)], v_buf.at[j, me], p1s.at[j], p1r.at[j], {"lon": q}
            ).start()
        v_buf[j, me] = s_buf[j, pl.ds(part_of(me, j), quarter), :]

    def deliver(j):
        all_of(v_buf, j, lons - 1, p1s.at[j], p1r.at[j]).wait_recv()
        offset = off[j]
        rest = lax.rem(offset, width)
        block = lax.rem(lax.div(offset, width), lons)
        begin = part_of(me, j)
        some = min(32, quarter)
        for first, size in pieces(0, quarter, some):
            place = lax.broadcasted_iota(jnp.int32, (size, levels), 0) + (begin + first)
            turn = jnp.where(place < rest, lax.rem(block + 1, lons), block)
            x = [v_buf[j, s, pl.ds(first, size), :] for s in range(lons)]
            bit = lons // 2
            while bit:
                mask = (turn & bit) != 0
                x = [jnp.where(mask, x[(d - bit) % lons], x[d]) for d in range(lons)]
                bit //= 2
            for d in range(lons):
                g_buf[j, d, pl.ds(first, size), :] = x[d]
        here = pl.ds(pl.multiple_of(2 * PAD + begin, PAD), quarter)
        west = pl.ds(PAD, PAD)
        east = pl.ds(2 * PAD + width, PAD)
        for k in range(1, lons):
            d = ring(k)
            remote(g_buf.at[j, d], f_buf.at[j, here], p2s.at[j], p2r.at[j], {"lon": d}).start()
        f_buf[j, here, :] = g_buf[j, me]
        part = lax.rem(me + j, lons)

        @pl.when(part == lons - 1)
        def _():
            for k in range(1, lons):
                src = g_buf.at[j, ring(k - 1), pl.ds(quarter - PAD, PAD)]
                remote(src, f_buf.at[j, west], ws.at[j], wr.at[j], {"lon": ring(k)}).start()
            f_buf[j, west, :] = g_buf[j, ring(-1), quarter - PAD :, :]

        @pl.when(part == 0)
        def _():
            for k in range(1, lons):
                src = g_buf.at[j, ring(k + 1), pl.ds(0, PAD)]
                remote(src, f_buf.at[j, east], es.at[j], er.at[j], {"lon": ring(k)}).start()
            f_buf[j, east, :] = g_buf[j, ring(1), :PAD, :]

    def edge_wait(j, send_sem, recv_sem, owner, count):
        block = f_buf.at[j, pl.ds(PAD, PAD * count)]
        return remote(block, block, send_sem, recv_sem, {"lon": ring(1)})

    def arrive(j):
        main = f_buf.at[j, pl.ds(2 * PAD, (lons - 1) * quarter)]
        remote(main, main, p2s.at[j], p2r.at[j], {"lon": ring(1)}).wait_recv()
        part = lax.rem(me + j, lons)

        @pl.when(part != lons - 1)
        def _():
            edge_wait(j, ws.at[j], wr.at[j], lons - 1, 1).wait_recv()

        @pl.when(part != 0)
        def _():
            edge_wait(j, es.at[j], er.at[j], 0, 1).wait_recv()

        c = cubic_weights(f_lon[j])
        for first, size in pieces(0, wide, 64):
            r_ext[deep + j, pl.ds(first, size), :] = sum(
                c[m] * f_buf[j, pl.ds(first + PAD - 1 + m, size), :] for m in range(4)
            )
        if j < deep:
            @pl.when(has_low)
            def _():
                low_copy(j).start()
        if j >= rows - deep:
            @pl.when(has_high)
            def _():
                high_copy(j).start()

    def low_copy(j):
        return remote(r_ext.at[deep + j], r_ext.at[deep + rows + j], fs.at[j], fr.at[j], below)

    def high_copy(j):
        m = j - (rows - deep)
        return remote(r_ext.at[deep + j], r_ext.at[m], fs.at[deep + m], fr.at[deep + m], above)

    def settle(j):
        all_of(g_buf, j, lons - 1, p2s.at[j], p2r.at[j]).wait_send()
        all_of(v_buf, j, lons - 1, p1s.at[j], p1r.at[j]).wait_send()
        part = lax.rem(me + j, lons)

        @pl.when(part == lons - 1)
        def _():
            edge_wait(j, ws.at[j], wr.at[j], lons - 1, lons - 1).wait_send()

        @pl.when(part == 0)
        def _():
            edge_wait(j, es.at[j], er.at[j], 0, lons - 1).wait_send()

    vc = vc_ref[...]
    up = jnp.where(lane < levels - 1, vc, 0.0)
    down = jnp.where(lane > 0, vc, 0.0)
    ws_refs, vs_refs = (w0, w1, w2), (v0, v1, v2)
    acc = [jnp.zeros((8, levels), F32) for _ in range(9)]

    def pack(e):
        high, low = split(inv_ext[e])
        packed[e, :levels, :levels] = high
        packed[e, :levels, levels:] = high
        packed[e, levels:, :levels] = low
        packed[e, levels:, levels:] = jnp.zeros((levels, levels), BF16)

    def solve(k, e, slot):
        both = lax.dot_general(
            lhs[slot], packed[e], (((1,), (1,)), ((), ())), preferred_element_type=F32
        )
        ws_refs[k][e - k, pl.ds(PAD, wide), :] = both[:, :levels] + both[:, levels:]

    def load_lhs(slot, first, size, v):
        high, low = split(v)
        lhs[slot, pl.ds(first, size), :levels] = high
        lhs[slot, pl.ds(first, size), levels:] = low

    def begin(e, slot):
        for first, size in pieces(0, wide, 64):
            load_lhs(slot, first, size, r_ext[e, pl.ds(first, size), :])
        solve(0, e, slot)

    def stencil(k, e, first, size):
        w = ws_refs[k]
        n = e - k
        m = met[e : e + 1, :]
        centre = w[n, pl.ds(first + PAD, size), :]
        result = (2.0 * m + 2.1 + 2.0 * vc) * centre
        result = result - m * (
            w[n, pl.ds(first + PAD + 1, size), :] + w[n, pl.ds(first + PAD - 1, size), :]
        )
        result = result - (w[n - 1, pl.ds(first + PAD, size), :] + w[n + 1, pl.ds(first + PAD, size), :])
        result = result - up * pltpu.roll(centre, levels - 1, 1)
        return result - down * pltpu.roll(centre, 1, 1)

    pairs = {0: ((0, "r", 0), (3, 0, 0)), 1: ((1, "r", 1), (4, 0, 1), (6, 1, 1)),
             2: ((2, "r", 2), (5, 0, 2), (7, 1, 2), (8, 2, 2))}

    def apply(k, e, slot):
        inside = deep <= e < deep + rows
        if k + 1 < ITERS:
            for first, size in pieces(0, wide, 64):
                v = stencil(k, e, first, size)
                load_lhs(slot, first, size, v)
                if inside:
                    vs_refs[k][e - deep, pl.ds(first, size), :] = v
            solve(k + 1, e, slot)
            if inside:
                for first, size in pieces(PAD, PAD + width, 64):
                    gather(k, e, first, size, vs_refs[k][e - deep, pl.ds(first, size), :])
        else:
            for first, size in pieces(PAD, PAD + width, 64):
                v = stencil(k, e, first, size)
                vs_refs[k][e - deep, pl.ds(first, size), :] = v
                gather(k, e, first, size, v)

    def gather(k, e, first, size, v):
        for n, p, q in pairs[k]:
            if p == "r":
                other = r_ext[e, pl.ds(first, size), :]
            elif p == k:
                other = v
            else:
                other = vs_refs[p][e - deep, pl.ds(first, size), :]
            acc[n] = acc[n] + fold(other * v)

    plain = lambda j: 1 <= j <= rows - 3
    edges = [j for j in range(rows) if j < deep or j >= rows - deep]
    order = [j for j in edges if plain(j)] + [j for j in edges if not plain(j)]
    order += [j for j in range(rows) if j not in order]
    waited = False
    sent_inv = False
    for j in order:
        if not plain(j) and not waited:
            waited = True

            @pl.when(has_low)
            def _():
                up_row.wait_recv()

            @pl.when(has_high)
            def _():
                down_rows.wait_recv()

        mix(j)
        spread(j)
        if not sent_inv:
            sent_inv = True
            matrices.wait()

            @pl.when(has_high)
            def _():
                up_inv.start()
                for copy in up_met:
                    copy.start()

            @pl.when(has_low)
            def _():
                down_inv.start()
                for copy in down_met:
                    copy.start()

    for e in range(deep, deep + rows):
        pack(e)
    for j in order:
        deliver(j)

    @pl.when(has_low)
    def _():
        up_inv.wait_recv()
        for copy in up_met:
            copy.wait_recv()

    @pl.when(has_high)
    def _():
        down_inv.wait_recv()
        for copy in down_met:
            copy.wait_recv()

    for e in list(range(deep)) + list(range(deep + rows, ext)):
        pack(e)

    done = {}
    slots = [0]

    def slot():
        slots[0] += 1
        return slots[0] % 2

    def ready():
        again = True
        while again:
            again = False
            for k in range(ITERS):
                for e in range(k + 1, ext - k - 1):
                    if ("v", k, e) not in done and all(("w", k, e + m) in done for m in (-1, 0, 1)):
                        apply(k, e, slot())
                        done["v", k, e] = True
                        if k + 1 < ITERS:
                            done["w", k + 1, e] = True
                        again = True

    def first_solve(e):
        begin(e, slot())
        done["w", 0, e] = True

    held = order[len(edges) :]
    for j in order[: len(edges)]:
        arrive(j)
    for j in order[: len(edges)]:
        first_solve(deep + j)
    ready()
    for j in held:
        arrive(j)
        first_solve(deep + j)
    ready()

    @pl.when(has_low)
    def _():
        for m in range(deep):
            high_copy(rows - deep + m).wait_recv()

    @pl.when(has_high)
    def _():
        for m in range(deep):
            low_copy(m).wait_recv()

    for e in list(range(deep)) + list(range(deep + rows, ext)):
        first_solve(e)
    ready()

    row = jnp.zeros((1, levels), F32)
    for n in range(9):
        row = jnp.where(lane == n, jnp.sum(jnp.sum(acc[n], axis=0, keepdims=True), axis=1, keepdims=True), row)
    part[...] = row
    every[mine] = row

    def tell(k, carry):
        remote(part, every.at[mine], rs, rr, peer_of(k)).start()
        return carry

    lax.fori_loop(1, devices, tell, 0)
    for j in range(rows):
        settle(j)

    @pl.when(has_high)
    def _():
        up_row.wait_send()
        up_inv.wait_send()
        for copy in up_met:
            copy.wait_send()
        for m in range(deep):
            high_copy(rows - deep + m).wait_send()

    @pl.when(has_low)
    def _():
        down_rows.wait_send()
        down_inv.wait_send()
        for copy in down_met:
            copy.wait_send()
        for m in range(deep):
            low_copy(m).wait_send()

    others = every.at[pl.ds(0, devices - 1)]
    totals = remote(others, others, rs, rr, {"lon": ring(1)})
    totals.wait_recv()
    totals.wait_send()
    tot[...] = jnp.broadcast_to(jnp.sum(every[...], axis=0), tot.shape)


def final_kernel(tot, r_ext, v0, v1, v2, w0, w1, w2, a_out, p_out, r_out, a_buf, p_buf, r_buf, sem):
    rows = v0.shape[0]
    levels = v0.shape[2]
    width = v0.shape[1] - 2 * PAD
    deep = DEEP
    total = tot[0:1, :]
    size = min(32, width)
    copies = []

    def ship(buf, out, c, n):
        at = pl.ds(c * size * rows, size * rows)
        copy = pltpu.make_async_copy(buf.at[at], out.at[at], sem.at[n, c])
        copy.start()
        copies.append(copy)

    for c in range(width // size):
        for j in range(rows):
            a_buf[pl.ds(c * size * rows + j, size, stride=rows), :] = r_ext[
                deep + j, pl.ds(PAD + c * size, size), :
            ]
        ship(a_buf, a_out, c, 0)
    rho, pi = coefficients([total[:, n : n + 1] for n in range(9)])
    rho = [jnp.broadcast_to(x, (8, levels))[0:1] for x in rho]
    pi = [jnp.broadcast_to(x, (8, levels))[0:1] for x in pi]
    for c in range(width // size):
        for j in range(rows):
            where = pl.ds(c * size * rows + j, size, stride=rows)
            at = pl.ds(PAD + c * size, size)
            wat = pl.ds(2 * PAD + c * size, size)
            p_buf[where, :] = (
                pi[0] * w0[deep + j, wat, :] + pi[1] * w1[deep - 1 + j, wat, :] + pi[2] * w2[deep - 2 + j, wat, :]
            )
            r_buf[where, :] = r_ext[deep + j, at, :] + (
                rho[0] * v0[j, at, :] + rho[1] * v1[j, at, :] + rho[2] * v2[j, at, :]
            )
        ship(p_buf, p_out, c, 1)
        ship(r_buf, r_out, c, 2)
    for copy in copies:
        copy.wait()


def body(tracer, offsets, frac_lon, frac_lat, frac_lev, metric, vertical_coef, inverses):
    width, rows, levels = tracer.shape
    lons, lats = lax.axis_size("lon"), lax.axis_size("lat")
    deep = DEEP
    ext, wide, quarter = rows + 2 * deep, width + 2 * PAD, width // lons
    devices = lons * lats
    dma = pltpu.SemaphoreType.DMA
    field = [shape(rows, wide, levels)] * 3
    sides = [shape(ext - 2 * k, wide + 2 * PAD, levels) for k in range(3)]
    arguments = (offsets, frac_lon, frac_lat, frac_lev, metric, vertical_coef.reshape(1, levels), tracer, inverses)
    arguments = [pltpu.with_memory_space_constraint(x, pltpu.HBM) for x in arguments]
    r_ext, v0, v1, v2, w0, w1, w2, tot = pl.pallas_call(
        functools.partial(step_kernel, lons, lats),
        out_shape=[shape(ext, wide, levels)] + field + sides + [shape(8, levels)],
        in_specs=[HBM] * 8,
        out_specs=[VM] * 8,
        scratch_shapes=[
            pltpu.VMEM((rows + 3, width, levels), F32),
            pltpu.VMEM((2, 2 * width, levels), F32),
            pltpu.VMEM((rows, width, levels), F32),
            pltpu.VMEM((rows, lons, quarter, levels), F32),
            pltpu.VMEM((rows, lons, quarter, levels), F32),
            pltpu.VMEM((rows, wide + 2 * PAD, levels), F32),
            pltpu.VMEM((ext, levels, levels), F32),
            pltpu.VMEM((ext, levels), F32),
            pltpu.VMEM((ext, 2 * levels, 2 * levels), BF16),
            pltpu.VMEM((2, wide, 2 * levels), BF16),
            pltpu.VMEM((1, levels), F32),
            pltpu.VMEM((devices, 1, levels), F32),
            pltpu.SMEM((rows,), jnp.int32),
        ]
        + [pltpu.SMEM((rows,), F32)] * 4
        + [
            pltpu.VMEM((1, levels), F32),
            dma((6,)),
            dma((rows,)),
            dma,
            dma((4,)),
            dma((4,)),
            dma((2 * deep,)),
            dma((2 * deep,)),
        ]
        + [dma((rows,))] * 8
        + [dma((2 * deep,))] * 2
        + [dma] * 2,
        compiler_params=pltpu.CompilerParams(
            collective_id=1, has_side_effects=True, vmem_limit_bytes=30 * 2**20
        ),
    )(*arguments)
    whole = shape(width * rows, levels)
    buffer = pltpu.VMEM((width * rows, levels), F32)
    outs = pl.pallas_call(
        final_kernel,
        out_shape=[whole] * 3,
        in_specs=[VM] * 8,
        out_specs=[ANY] * 3,
        scratch_shapes=[buffer] * 3 + [dma((3, width // min(32, width)))],
        compiler_params=pltpu.CompilerParams(vmem_limit_bytes=20 * 2**20),
    )(tot, r_ext, v0, v1, v2, w0, w1, w2)
    return tuple(x.reshape(width, rows, levels) for x in outs)


def solution(mesh):
    cube = P("lon", "lat", None)
    in_specs = (cube, P("lat"), P("lat"), P("lat"), P("lat"), P("lat"), P(), P("lat", None, None))
    return jax.shard_map(
        body, mesh=mesh, in_specs=in_specs, out_specs=(cube, cube, cube), check_vma=False
    )
```

```python
import functools

import jax
import jax.numpy as jnp
from jax import lax
from jax.experimental import pallas as pl
from jax.experimental.pallas import tpu as pltpu
from jax.sharding import PartitionSpec as P

ITERS = 3
DEEP = ITERS
PAD = 8
VM = pl.BlockSpec(memory_space=pltpu.VMEM)
ANY = pl.BlockSpec(memory_space=pl.ANY)
HBM = pl.BlockSpec(memory_space=pltpu.HBM)
F32 = jnp.float32
BF16 = jnp.bfloat16
MESH = pl.DeviceIdType.MESH


def cubic_weights(f):
    return (
        -f * (f - 1.0) * (f - 2.0) * (1.0 / 6.0),
        (f + 1.0) * (f - 1.0) * (f - 2.0) * 0.5,
        -(f + 1.0) * f * (f - 2.0) * 0.5,
        (f + 1.0) * f * (f - 1.0) * (1.0 / 6.0),
    )


def shape(*dims, dtype=F32):
    return jax.ShapeDtypeStruct(dims, dtype)


def signal(sem, peer):
    pl.semaphore_signal(sem, inc=1, device_id=peer, device_id_type=MESH)


def remote(src, dst, send_sem, recv_sem, peer):
    return pltpu.make_async_remote_copy(
        src_ref=src,
        dst_ref=dst,
        send_sem=send_sem,
        recv_sem=recv_sem,
        device_id=peer,
        device_id_type=MESH,
    )


def split(x):
    high = x.astype(BF16)
    return high, (x - high.astype(F32)).astype(BF16)


def pieces(first, last, size):
    out = []
    while first < last:
        step = size if last - first < 2 * size else size
        step = min(step, last - first)
        out.append((first, step))
        first += step
    return out


def fold(x):
    return jnp.sum(x.reshape(x.shape[0] // 8, 8, x.shape[1]), axis=0)


def coefficients(t):
    right = t[:3]
    gram = [[t[3], t[4], t[5]], [t[4], t[6], t[7]], [t[5], t[7], t[8]]]
    zero = jnp.zeros_like(t[0])

    def form(p, q):
        total = zero
        for k in range(3):
            for l in range(3):
                if p[k] is not None and q[l] is not None:
                    total = total + p[k] * q[l] * gram[k][l]
        return total

    def add(p, s, q):
        return [x if y is None else (s * y if x is None else x + s * y) for x, y in zip(p, q)]

    q = [[zero + 1.0, None, None]]
    rho, pi = [None] * 3, [None] * 3
    squares = [form(q[0], q[0])]
    for i in range(ITERS):
        along = form(q[i], rho)
        for k in range(3):
            if q[i][k] is not None:
                along = along + q[i][k] * right[k]
        alpha = along / squares[i]
        pi = add(pi, alpha, q[i])
        rho = add(rho, -alpha, q[i])
        if i + 1 < ITERS:
            z = [zero + 1.0, rho[0], rho[1]]
            new = z
            for l in range(i + 1):
                new = add(new, -form(z, q[l]) / squares[l], q[l])
            q.append(new)
            squares.append(form(new, new))
    return rho, pi


def step_kernel(lons, lats, *refs):
    scalars, (tracer, inv), refs = refs[:6], refs[6:8], refs[8:]
    flat, tot, refs = refs[:7], refs[7], refs[8:]
    (r_ext, v0, v1, v2, w0, w1, w2, z0, z1, z2), refs = refs[:10], refs[10:]
    (t, double, s_buf, v_buf, g_buf, f_buf, inv_ext, met), refs = refs[:8], refs[8:]
    (column, packed, extra, lhs, part, every), refs = refs[:6], refs[6:]
    (off, f_lon, f_lat, f_lev, metric, vc_ref, c_sem), refs = refs[:7], refs[7:]
    (t_sem, i_sem, hs, hr, ns, nr, p1s, p1r, p2s, p2r, ws, wr, es, er, fs, fr, rs, rr) = refs
    width, rows, levels = tracer.shape
    quarter = width // lons
    deep = DEEP
    ext, wide = rows + 2 * deep, width + 2 * PAD
    me, lat = lax.axis_index("lon"), lax.axis_index("lat")
    ring = lambda k: lax.rem(me + (k + lons), lons)
    has_low, has_high = lat > 0, lat < lats - 1
    below = {"lat": lax.max(lat - 1, 0)}
    above = {"lat": lax.min(lat + 1, lats - 1)}
    devices = lons * lats
    mine = me * lats + lat
    lane = lax.broadcasted_iota(jnp.int32, (1, levels), 1)

    def peer_of(k):
        index = lax.rem(mine + k, devices)
        return {"lon": lax.div(index, lats), "lat": lax.rem(index, lats)}

    first_rows = [rows - 1, 0, 1] + list(range(2, rows - 1))
    loads = {j: pltpu.make_async_copy(tracer.at[:, j, :], t.at[j + 1], t_sem.at[j]) for j in range(rows)}
    for j in first_rows:
        loads[j].start()
    fetches = [
        pltpu.make_async_copy(src, dst, c_sem.at[n])
        for n, (src, dst) in enumerate(zip(scalars, (off, f_lon, f_lat, f_lev, metric, vc_ref)))
    ]
    for copy in fetches:
        copy.start()
    matrices = pltpu.make_async_copy(inv, inv_ext.at[pl.ds(deep, rows)], i_sem)
    matrices.start()

    barrier = pltpu.get_barrier_semaphore()
    lax.fori_loop(1, devices, lambda k, c: (signal(barrier, peer_of(k)), c)[1], 0)

    for copy in fetches:
        copy.wait()
    for j in range(rows):
        met[deep + j : deep + j + 1, :] = jnp.full((1, levels), metric[j], F32)

    def clear_pads():
        for j in range(rows):
            f_buf[j, :PAD, :] = jnp.zeros((PAD, levels), F32)
            f_buf[j, wide + PAD :, :] = jnp.zeros((PAD, levels), F32)
        for w in (w0, w1, w2):
            for e in range(w.shape[0]):
                w[e, :PAD, :] = jnp.zeros((PAD, levels), F32)
                w[e, wide + PAD :, :] = jnp.zeros((PAD, levels), F32)

    def clear(ref, first, count):
        ref[first : first + count] = jnp.zeros((count,) + ref.shape[1:], F32)

    @pl.when(jnp.logical_not(has_low))
    def _():
        clear(t, 0, 1)
        clear(r_ext, 0, deep)
        clear(inv_ext, 0, deep)
        met[:deep, :] = jnp.zeros((deep, levels), F32)

    @pl.when(jnp.logical_not(has_high))
    def _():
        clear(t, rows + 1, 2)
        clear(r_ext, deep + rows, deep)
        clear(inv_ext, deep + rows, deep)
        met[deep + rows : ext, :] = jnp.zeros((deep, levels), F32)

    up_row = remote(t.at[rows], t.at[0], hs.at[0], hr.at[0], above)
    down_rows = remote(t.at[pl.ds(1, 2)], t.at[pl.ds(rows + 1, 2)], hs.at[1], hr.at[1], below)
    up_inv = remote(inv_ext.at[pl.ds(rows, deep)], inv_ext.at[pl.ds(0, deep)], hs.at[2], hr.at[2], above)
    down_inv = remote(
        inv_ext.at[pl.ds(deep, deep)], inv_ext.at[pl.ds(deep + rows, deep)], hs.at[3], hr.at[3], below
    )
    up_met = [remote(met.at[rows + m], met.at[m], ns.at[m], nr.at[m], above) for m in range(deep)]
    down_met = [
        remote(met.at[deep + m], met.at[deep + rows + m], ns.at[deep + m], nr.at[deep + m], below)
        for m in range(deep)
    ]
    for j in first_rows[:3]:
        loads[j].wait()
    pl.semaphore_wait(barrier, devices - 1)

    @pl.when(has_high)
    def _():
        up_row.start()

    @pl.when(has_low)
    def _():
        down_rows.start()

    for j in first_rows[3:]:
        loads[j].wait()

    def mix(j):
        a = cubic_weights(f_lat[j])
        b = cubic_weights(f_lev[j])
        taps = {m: jnp.where((lane + m >= 0) & (lane + m < levels), b[m + 1], 0.0) for m in (-1, 1, 2)}
        buffer = double.at[j % 2]
        for first, size in pieces(0, width, 64):
            at = pl.ds(first, size)
            x = a[0] * t[j, at, :] + a[1] * t[j + 1, at, :] + a[2] * t[j + 2, at, :] + a[3] * t[j + 3, at, :]
            total = b[1] * x
            for m in (-1, 1, 2):
                total = total + taps[m] * pltpu.roll(x, (-m) % levels, 1)
            buffer[at, :] = total
            buffer[pl.ds(width + first, size), :] = total
        start = width - lax.rem(off[j], width)
        for first, size in pieces(0, width, 64):
            s_buf[j, pl.ds(first, size), :] = buffer[pl.ds(start + first, size), :]

    def part_of(device, j):
        return pl.multiple_of(lax.rem(device + j, lons) * quarter, quarter)

    def all_of(ref, j, count, send_sem, recv_sem):
        return remote(ref.at[j, pl.ds(0, count)], ref.at[j, pl.ds(0, count)], send_sem, recv_sem, {"lon": ring(1)})

    def spread(j):
        for k in range(1, lons):
            q = ring(k)
            remote(
                s_buf.at[j, pl.ds(part_of(q, j), quarter)], v_buf.at[j, me], p1s.at[j], p1r.at[j], {"lon": q}
            ).start()
        v_buf[j, me] = s_buf[j, pl.ds(part_of(me, j), quarter), :]

    def deliver(j):
        all_of(v_buf, j, lons - 1, p1s.at[j], p1r.at[j]).wait_recv()
        offset = off[j]
        rest = lax.rem(offset, width)
        block = lax.rem(lax.div(offset, width), lons)
        begin = part_of(me, j)
        some = min(32, quarter)
        for first, size in pieces(0, quarter, some):
            place = lax.broadcasted_iota(jnp.int32, (size, levels), 0) + (begin + first)
            turn = jnp.where(place < rest, lax.rem(block + 1, lons), block)
            x = [v_buf[j, s, pl.ds(first, size), :] for s in range(lons)]
            bit = lons // 2
            while bit:
                mask = (turn & bit) != 0
                x = [jnp.where(mask, x[(d - bit) % lons], x[d]) for d in range(lons)]
                bit //= 2
            for d in range(lons):
                g_buf[j, d, pl.ds(first, size), :] = x[d]
        here = pl.ds(pl.multiple_of(2 * PAD + begin, PAD), quarter)
        west = pl.ds(PAD, PAD)
        east = pl.ds(2 * PAD + width, PAD)
        for k in range(1, lons):
            d = ring(k)
            remote(g_buf.at[j, d], f_buf.at[j, here], p2s.at[j], p2r.at[j], {"lon": d}).start()
        f_buf[j, here, :] = g_buf[j, me]
        part = lax.rem(me + j, lons)

        @pl.when(part == lons - 1)
        def _():
            for k in range(1, lons):
                src = g_buf.at[j, ring(k - 1), pl.ds(quarter - PAD, PAD)]
                remote(src, f_buf.at[j, west], ws.at[j], wr.at[j], {"lon": ring(k)}).start()
            f_buf[j, west, :] = g_buf[j, ring(-1), quarter - PAD :, :]

        @pl.when(part == 0)
        def _():
            for k in range(1, lons):
                src = g_buf.at[j, ring(k + 1), pl.ds(0, PAD)]
                remote(src, f_buf.at[j, east], es.at[j], er.at[j], {"lon": ring(k)}).start()
            f_buf[j, east, :] = g_buf[j, ring(1), :PAD, :]

    def edge_wait(j, send_sem, recv_sem, owner, count):
        block = f_buf.at[j, pl.ds(PAD, PAD * count)]
        return remote(block, block, send_sem, recv_sem, {"lon": ring(1)})

    def arrive(j):
        main = f_buf.at[j, pl.ds(2 * PAD, (lons - 1) * quarter)]
        remote(main, main, p2s.at[j], p2r.at[j], {"lon": ring(1)}).wait_recv()
        part = lax.rem(me + j, lons)

        @pl.when(part != lons - 1)
        def _():
            edge_wait(j, ws.at[j], wr.at[j], lons - 1, 1).wait_recv()

        @pl.when(part != 0)
        def _():
            edge_wait(j, es.at[j], er.at[j], 0, 1).wait_recv()

        c = cubic_weights(f_lon[j])
        for first, size in pieces(0, wide, 64):
            r_ext[deep + j, pl.ds(first, size), :] = sum(
                c[m] * f_buf[j, pl.ds(first + PAD - 1 + m, size), :] for m in range(4)
            )
        if j < deep:
            @pl.when(has_low)
            def _():
                low_copy(j).start()
        if j >= rows - deep:
            @pl.when(has_high)
            def _():
                high_copy(j).start()

    def low_copy(j):
        return remote(r_ext.at[deep + j], r_ext.at[deep + rows + j], fs.at[j], fr.at[j], below)

    def high_copy(j):
        m = j - (rows - deep)
        return remote(r_ext.at[deep + j], r_ext.at[m], fs.at[deep + m], fr.at[deep + m], above)

    def settle(j):
        all_of(g_buf, j, lons - 1, p2s.at[j], p2r.at[j]).wait_send()
        all_of(v_buf, j, lons - 1, p1s.at[j], p1r.at[j]).wait_send()
        part = lax.rem(me + j, lons)

        @pl.when(part == lons - 1)
        def _():
            edge_wait(j, ws.at[j], wr.at[j], lons - 1, lons - 1).wait_send()

        @pl.when(part == 0)
        def _():
            edge_wait(j, es.at[j], er.at[j], 0, lons - 1).wait_send()

    ws_refs, vs_refs, zs_refs = (w0, w1, w2), (v0, v1, v2), (z0, z1, z2)
    acc = [jnp.zeros((8, levels), F32) for _ in range(9)]
    lines = 32

    def turn_coefficients():
        tall = jnp.broadcast_to(vc_ref[...], (levels, levels)).T
        place = lax.broadcasted_iota(jnp.int32, (levels, levels), 0)
        column[0] = 2.1 + 2.0 * tall
        column[1] = jnp.where(place < levels - 1, tall, 0.0)
        column[2] = jnp.where(place > 0, tall, 0.0)

    def pack(e):
        matrix = inv_ext[e]
        applied = column[0] * matrix - column[1] * pltpu.roll(matrix, levels - 1, 0)
        applied = applied - column[2] * pltpu.roll(matrix, 1, 0)
        for n, x in enumerate((matrix, applied)):
            high, low = split(x)
            at = pl.ds(n * levels, levels)
            packed[e, at, :levels] = high
            packed[e, at, levels:] = high
            extra[e, at, :] = low

    def solve(k, e, slot):
        dims = (((1,), (1,)), ((), ()))
        both = lax.dot_general(lhs[slot], packed[e], dims, preferred_element_type=F32)
        both = both + lax.dot_general(lhs[slot, :, :levels], extra[e], dims, preferred_element_type=F32)
        ws_refs[k][e - k, pl.ds(PAD, wide), :] = both[:, :levels]
        if k < e < ext - k - 1:
            zs_refs[k][e - k - 1] = both[:, levels:]

    def load_lhs(slot, first, size, v):
        high, low = split(v)
        lhs[slot, pl.ds(first, size), :levels] = high
        lhs[slot, pl.ds(first, size), levels:] = low

    def begin(e, slot):
        for first, size in pieces(0, wide, lines):
            load_lhs(slot, first, size, r_ext[e, pl.ds(first, size), :])
        solve(0, e, slot)

    def stencil(k, e, first, size):
        w = ws_refs[k]
        n = e - k
        m = met[e : e + 1, :]
        at = pl.ds(first + PAD, size)
        result = zs_refs[k][n - 1, pl.ds(first, size), :] + (2.0 * m) * w[n, at, :]
        result = result - m * (
            w[n, pl.ds(first + PAD + 1, size), :] + w[n, pl.ds(first + PAD - 1, size), :]
        )
        return result - (w[n - 1, at, :] + w[n + 1, at, :])

    pairs = {0: ((0, "r", 0), (3, 0, 0)), 1: ((1, "r", 1), (4, 0, 1), (6, 1, 1)),
             2: ((2, "r", 2), (5, 0, 2), (7, 1, 2), (8, 2, 2))}

    def apply(k, e, slot):
        inside = deep <= e < deep + rows
        if k + 1 < ITERS:
            for first, size in pieces(0, wide, lines):
                v = stencil(k, e, first, size)
                load_lhs(slot, first, size, v)
                if inside:
                    vs_refs[k][e - deep, pl.ds(first, size), :] = v
            solve(k + 1, e, slot)
            if inside:
                for first, size in pieces(PAD, PAD + width, lines):
                    gather(k, e, first, size, vs_refs[k][e - deep, pl.ds(first, size), :])
        else:
            for first, size in pieces(PAD, PAD + width, lines):
                v = stencil(k, e, first, size)
                vs_refs[k][e - deep, pl.ds(first, size), :] = v
                gather(k, e, first, size, v)

    def gather(k, e, first, size, v):
        for n, p, q in pairs[k]:
            if p == "r":
                other = r_ext[e, pl.ds(first, size), :]
            elif p == k:
                other = v
            else:
                other = vs_refs[p][e - deep, pl.ds(first, size), :]
            acc[n] = acc[n] + fold(other * v)

    plain = lambda j: 1 <= j <= rows - 3
    edges = [j for j in range(rows) if j < deep or j >= rows - deep]
    order = [j for j in edges if plain(j)] + [j for j in edges if not plain(j)]
    order += [j for j in range(rows) if j not in order]
    outer = sorted(edges, key=lambda j: min(j, rows - 1 - j))
    later = outer + [j for j in range(rows) if j not in outer]
    waited = False
    sent_inv = False
    for j in order:
        if not plain(j) and not waited:
            waited = True

            @pl.when(has_low)
            def _():
                up_row.wait_recv()

            @pl.when(has_high)
            def _():
                down_rows.wait_recv()

        mix(j)
        spread(j)
        if not sent_inv:
            sent_inv = True
            matrices.wait()

            @pl.when(has_high)
            def _():
                up_inv.start()
                for copy in up_met:
                    copy.start()

            @pl.when(has_low)
            def _():
                down_inv.start()
                for copy in down_met:
                    copy.start()

    clear_pads()
    turn_coefficients()
    for j in later:
        deliver(j)
    for e in range(deep, deep + rows):
        pack(e)

    @pl.when(has_low)
    def _():
        up_inv.wait_recv()
        for copy in up_met:
            copy.wait_recv()

    @pl.when(has_high)
    def _():
        down_inv.wait_recv()
        for copy in down_met:
            copy.wait_recv()

    for e in list(range(deep)) + list(range(deep + rows, ext)):
        pack(e)

    done = {}
    slots = [0]

    def slot():
        slots[0] += 1
        return slots[0] % 2

    def ready():
        again = True
        while again:
            again = False
            for k in range(ITERS):
                for e in range(k + 1, ext - k - 1):
                    if ("v", k, e) not in done and all(("w", k, e + m) in done for m in (-1, 0, 1)):
                        apply(k, e, slot())
                        done["v", k, e] = True
                        if k + 1 < ITERS:
                            done["w", k + 1, e] = True
                        again = True

    def first_solve(e):
        begin(e, slot())
        done["w", 0, e] = True

    def halo_rows(m):
        @pl.when(has_low)
        def _():
            high_copy(rows - 1 - m).wait_recv()

        @pl.when(has_high)
        def _():
            low_copy(m).wait_recv()

        for e in (deep - 1 - m, deep + rows + m):
            first_solve(e)

    for n, j in enumerate(outer):
        arrive(j)
        first_solve(deep + j)
        if n % 2 == 1 and n >= 3:
            halo_rows(n // 2 - 1)
        ready()
    for j in later[len(outer) :]:
        arrive(j)
        first_solve(deep + j)
        ready()
    halo_rows(deep - 1)
    ready()

    row = jnp.zeros((1, levels), F32)
    for n in range(9):
        row = jnp.where(lane == n, jnp.sum(jnp.sum(acc[n], axis=0, keepdims=True), axis=1, keepdims=True), row)
    part[...] = row
    every[mine] = row

    def tell(a, b):
        to = {"lon": ring(a), "lat": lax.rem(lat + b, lats)}
        remote(part, every.at[mine], rs, rr, to).start()

    def tell_rest(k, carry):
        remote(part, every.at[mine], rs, rr, peer_of(k)).start()
        return carry

    if devices <= 64:
        far = lambda n, count: sorted(range(n), key=lambda k: abs(k - n // 2))
        for b in far(lats, lats):
            for a in far(lons, lons):
                if a or b:
                    tell(a, b)
    else:
        lax.fori_loop(1, devices, tell_rest, 0)
    for j in range(rows):
        where = pl.ds(j, width, stride=rows)
        flat[0][where, :] = r_ext[deep + j, pl.ds(PAD, width), :]
        for k in range(ITERS):
            flat[1 + k][where, :] = vs_refs[k][j, pl.ds(PAD, width), :]
            flat[4 + k][where, :] = ws_refs[k][deep + j - k, pl.ds(2 * PAD, width), :]
    for j in range(rows):
        settle(j)

    @pl.when(has_high)
    def _():
        up_row.wait_send()
        up_inv.wait_send()
        for copy in up_met:
            copy.wait_send()
        for m in range(deep):
            high_copy(rows - deep + m).wait_send()

    @pl.when(has_low)
    def _():
        down_rows.wait_send()
        down_inv.wait_send()
        for copy in down_met:
            copy.wait_send()
        for m in range(deep):
            low_copy(m).wait_send()

    others = every.at[pl.ds(0, devices - 1)]
    totals = remote(others, others, rs, rr, {"lon": ring(1)})
    totals.wait_recv()
    totals.wait_send()
    tot[...] = jnp.broadcast_to(jnp.sum(every[...], axis=0), tot.shape)


def final_kernel(size, tot, r, v0, v1, v2, w0, w1, w2, a_out, p_out, r_out, p_buf, r_buf, a_sem, sem):
    advected = pltpu.make_async_copy(r, a_out, a_sem)
    advected.start()
    total = tot[0:1, :]
    rho, pi = coefficients([jnp.broadcast_to(total[:, n : n + 1], total.shape) for n in range(9)])
    copies = []
    for c in range(r.shape[0] // size):
        at = pl.ds(c * size, size)
        p_buf[at, :] = pi[0] * w0[at, :] + pi[1] * w1[at, :] + pi[2] * w2[at, :]
        r_buf[at, :] = r[at, :] + (rho[0] * v0[at, :] + rho[1] * v1[at, :] + rho[2] * v2[at, :])
        for n, (src, dst) in enumerate(((p_buf, p_out), (r_buf, r_out))):
            copy = pltpu.make_async_copy(src.at[at], dst.at[at], sem.at[n, c])
            copy.start()
            copies.append(copy)
    for copy in copies:
        copy.wait()
    advected.wait()


def body(tracer, offsets, frac_lon, frac_lat, frac_lev, metric, vertical_coef, inverses):
    width, rows, levels = tracer.shape
    lons, lats = lax.axis_size("lon"), lax.axis_size("lat")
    deep = DEEP
    ext, wide, quarter = rows + 2 * deep, width + 2 * PAD, width // lons
    devices = lons * lats
    dma = pltpu.SemaphoreType.DMA
    whole = shape(width * rows, levels)
    field = [pltpu.VMEM((rows, wide, levels), F32)] * 3
    sides = [pltpu.VMEM((ext - 2 * k, wide + 2 * PAD, levels), F32) for k in range(3)]
    verticals = [pltpu.VMEM((ext - 2 * k - 2, wide, levels), F32) for k in range(3)]
    arguments = (offsets, frac_lon, frac_lat, frac_lev, metric, vertical_coef.reshape(1, levels), tracer, inverses)
    arguments = [pltpu.with_memory_space_constraint(x, pltpu.HBM) for x in arguments]
    *flat, tot = pl.pallas_call(
        functools.partial(step_kernel, lons, lats),
        out_shape=[whole] * 7 + [shape(8, levels)],
        in_specs=[HBM] * 8,
        out_specs=[VM] * 8,
        scratch_shapes=[pltpu.VMEM((ext, wide, levels), F32)]
        + field
        + sides
        + verticals
        + [
            pltpu.VMEM((rows + 3, width, levels), F32),
            pltpu.VMEM((2, 2 * width, levels), F32),
            pltpu.VMEM((rows, width, levels), F32),
            pltpu.VMEM((rows, lons, quarter, levels), F32),
            pltpu.VMEM((rows, lons, quarter, levels), F32),
            pltpu.VMEM((rows, wide + 2 * PAD, levels), F32),
            pltpu.VMEM((ext, levels, levels), F32),
            pltpu.VMEM((ext, levels), F32),
            pltpu.VMEM((3, levels, levels), F32),
            pltpu.VMEM((ext, 2 * levels, 2 * levels), BF16),
            pltpu.VMEM((ext, 2 * levels, levels), BF16),
            pltpu.VMEM((2, wide, 2 * levels), BF16),
            pltpu.VMEM((1, levels), F32),
            pltpu.VMEM((devices, 1, levels), F32),
            pltpu.SMEM((rows,), jnp.int32),
        ]
        + [pltpu.SMEM((rows,), F32)] * 4
        + [
            pltpu.VMEM((1, levels), F32),
            dma((6,)),
            dma((rows,)),
            dma,
            dma((4,)),
            dma((4,)),
            dma((2 * deep,)),
            dma((2 * deep,)),
        ]
        + [dma((rows,))] * 8
        + [dma((2 * deep,))] * 2
        + [dma] * 2,
        compiler_params=pltpu.CompilerParams(
            collective_id=1, has_side_effects=True, vmem_limit_bytes=40 * 2**20
        ),
    )(*arguments)
    size = min(256, width * rows)
    outs = pl.pallas_call(
        functools.partial(final_kernel, size),
        out_shape=[whole] * 3,
        in_specs=[VM] * 8,
        out_specs=[ANY] * 3,
        scratch_shapes=[pltpu.VMEM((width * rows, levels), F32)] * 2 + [dma, dma((2, width * rows // size))],
        compiler_params=pltpu.CompilerParams(vmem_limit_bytes=16 * 2**20),
    )(tot, *flat)
    return tuple(x.reshape(width, rows, levels) for x in outs)


def solution(mesh):
    cube = P("lon", "lat", None)
    in_specs = (cube, P("lat"), P("lat"), P("lat"), P("lat"), P("lat"), P(), P("lat", None, None))
    return jax.shard_map(
        body, mesh=mesh, in_specs=in_specs, out_specs=(cube, cube, cube), check_vma=False
    )
```

```python
import functools

import jax
import jax.numpy as jnp
from jax import lax
from jax.experimental import pallas as pl
from jax.experimental.pallas import tpu as pltpu
from jax.sharding import PartitionSpec as P

ITERS = 3
DEEP = ITERS
PAD = 8
VM = pl.BlockSpec(memory_space=pltpu.VMEM)
ANY = pl.BlockSpec(memory_space=pl.ANY)
HBM = pl.BlockSpec(memory_space=pltpu.HBM)
F32 = jnp.float32
BF16 = jnp.bfloat16
MESH = pl.DeviceIdType.MESH


def cubic_weights(f):
    return (
        -f * (f - 1.0) * (f - 2.0) * (1.0 / 6.0),
        (f + 1.0) * (f - 1.0) * (f - 2.0) * 0.5,
        -(f + 1.0) * f * (f - 2.0) * 0.5,
        (f + 1.0) * f * (f - 1.0) * (1.0 / 6.0),
    )


def shape(*dims, dtype=F32):
    return jax.ShapeDtypeStruct(dims, dtype)


def signal(sem, peer):
    pl.semaphore_signal(sem, inc=1, device_id=peer, device_id_type=MESH)


def remote(src, dst, send_sem, recv_sem, peer):
    return pltpu.make_async_remote_copy(
        src_ref=src,
        dst_ref=dst,
        send_sem=send_sem,
        recv_sem=recv_sem,
        device_id=peer,
        device_id_type=MESH,
    )


def split(x):
    high = x.astype(BF16)
    return high, (x - high.astype(F32)).astype(BF16)


def pieces(first, last, size):
    out = []
    while first < last:
        step = size if last - first < 2 * size else size
        step = min(step, last - first)
        out.append((first, step))
        first += step
    return out


def fold(x):
    return jnp.sum(x.reshape(x.shape[0] // 8, 8, x.shape[1]), axis=0)


def coefficients(t):
    right = t[:3]
    gram = [[t[3], t[4], t[5]], [t[4], t[6], t[7]], [t[5], t[7], t[8]]]
    zero = jnp.zeros_like(t[0])

    def form(p, q):
        total = zero
        for k in range(3):
            for l in range(3):
                if p[k] is not None and q[l] is not None:
                    total = total + p[k] * q[l] * gram[k][l]
        return total

    def add(p, s, q):
        return [x if y is None else (s * y if x is None else x + s * y) for x, y in zip(p, q)]

    q = [[zero + 1.0, None, None]]
    rho, pi = [None] * 3, [None] * 3
    squares = [form(q[0], q[0])]
    for i in range(ITERS):
        along = form(q[i], rho)
        for k in range(3):
            if q[i][k] is not None:
                along = along + q[i][k] * right[k]
        alpha = along / squares[i]
        pi = add(pi, alpha, q[i])
        rho = add(rho, -alpha, q[i])
        if i + 1 < ITERS:
            z = [zero + 1.0, rho[0], rho[1]]
            new = z
            for l in range(i + 1):
                new = add(new, -form(z, q[l]) / squares[l], q[l])
            q.append(new)
            squares.append(form(new, new))
    return rho, pi


def step_kernel(lons, lats, *refs):
    scalars, (tracer, inv), refs = refs[:6], refs[6:8], refs[8:]
    flat, tot, refs = refs[:7], refs[7], refs[8:]
    (r_ext, v0, v1, v2, w0, w1, w2, z0, z1, z2), refs = refs[:10], refs[10:]
    (t, double, s_buf, v_buf, g_buf, f_buf, inv_ext, met), refs = refs[:8], refs[8:]
    (column, packed, extra, lhs, part, every), refs = refs[:6], refs[6:]
    (off, f_lon, f_lat, f_lev, metric, vc_ref, c_sem), refs = refs[:7], refs[7:]
    (t_sem, i_sem, hs, hr, ns, nr, p1s, p1r, p2s, p2r, fs, fr, rs, rr) = refs
    width, rows, levels = tracer.shape
    quarter = width // lons
    deep = DEEP
    ext, wide = rows + 2 * deep, width + 2 * PAD
    me, lat = lax.axis_index("lon"), lax.axis_index("lat")
    ring = lambda k: lax.rem(me + (k + lons), lons)
    has_low, has_high = lat > 0, lat < lats - 1
    below = {"lat": lax.max(lat - 1, 0)}
    above = {"lat": lax.min(lat + 1, lats - 1)}
    devices = lons * lats
    mine = me * lats + lat
    lane = lax.broadcasted_iota(jnp.int32, (1, levels), 1)

    def peer_of(k):
        index = lax.rem(mine + k, devices)
        return {"lon": lax.div(index, lats), "lat": lax.rem(index, lats)}

    first_rows = [0, 1, 2, 3, rows - 1] + list(range(4, rows - 1))
    loads = {j: pltpu.make_async_copy(tracer.at[:, j, :], t.at[j + 1], t_sem.at[j]) for j in range(rows)}
    for j in first_rows:
        loads[j].start()
    fetches = [
        pltpu.make_async_copy(src, dst, c_sem.at[n])
        for n, (src, dst) in enumerate(zip(scalars, (off, f_lon, f_lat, f_lev, metric, vc_ref)))
    ]
    for copy in fetches:
        copy.start()
    matrices = pltpu.make_async_copy(inv, inv_ext.at[pl.ds(deep, rows)], i_sem)
    matrices.start()

    barrier = pltpu.get_barrier_semaphore()
    def others():
        far = lambda n: sorted(range(n), key=lambda k: abs(k - n // 2))
        for b in far(lats):
            for a in far(lons):
                if a or b:
                    yield {"lon": ring(a), "lat": lax.rem(lat + b, lats)}

    unrolled = devices <= 64
    if unrolled:
        for peer in others():
            signal(barrier, peer)
    else:
        lax.fori_loop(1, devices, lambda k, c: (signal(barrier, peer_of(k)), c)[1], 0)

    def clear_pads():
        for j in range(rows):
            f_buf[j, :PAD, :] = jnp.zeros((PAD, levels), F32)
            f_buf[j, wide + PAD :, :] = jnp.zeros((PAD, levels), F32)
        for w in (w0, w1, w2):
            for e in range(w.shape[0]):
                w[e, :PAD, :] = jnp.zeros((PAD, levels), F32)
                w[e, wide + PAD :, :] = jnp.zeros((PAD, levels), F32)

    def clear(ref, first, count):
        ref[first : first + count] = jnp.zeros((count,) + ref.shape[1:], F32)

    def clear_sides():
        @pl.when(jnp.logical_not(has_low))
        def _():
            clear(r_ext, 0, deep)
            clear(inv_ext, 0, deep)
            met[:deep, :] = jnp.zeros((deep, levels), F32)

        @pl.when(jnp.logical_not(has_high))
        def _():
            clear(r_ext, deep + rows, deep)
            clear(inv_ext, deep + rows, deep)
            met[deep + rows : ext, :] = jnp.zeros((deep, levels), F32)

    up_row = remote(t.at[rows], t.at[0], hs.at[0], hr.at[0], above)
    down_rows = remote(t.at[pl.ds(1, 2)], t.at[pl.ds(rows + 1, 2)], hs.at[1], hr.at[1], below)
    up_inv = remote(inv_ext.at[pl.ds(rows, deep)], inv_ext.at[pl.ds(0, deep)], hs.at[2], hr.at[2], above)
    down_inv = remote(
        inv_ext.at[pl.ds(deep, deep)], inv_ext.at[pl.ds(deep + rows, deep)], hs.at[3], hr.at[3], below
    )
    up_met = [remote(met.at[rows + m], met.at[m], ns.at[m], nr.at[m], above) for m in range(deep)]
    down_met = [
        remote(met.at[deep + m], met.at[deep + rows + m], ns.at[deep + m], nr.at[deep + m], below)
        for m in range(deep)
    ]
    def mix(j):
        a = cubic_weights(f_lat[j])
        b = cubic_weights(f_lev[j])
        taps = {m: jnp.where((lane + m >= 0) & (lane + m < levels), b[m + 1], 0.0) for m in (-1, 1, 2)}
        buffer = double.at[j % 2]
        for first, size in pieces(0, width, 64):
            at = pl.ds(first, size)
            x = a[0] * t[j, at, :] + a[1] * t[j + 1, at, :] + a[2] * t[j + 2, at, :] + a[3] * t[j + 3, at, :]
            total = b[1] * x
            for m in (-1, 1, 2):
                total = total + taps[m] * pltpu.roll(x, (-m) % levels, 1)
            buffer[at, :] = total
            buffer[pl.ds(width + first, size), :] = total
        start = width - lax.rem(off[j], width)
        for first, size in pieces(0, width, 64):
            s_buf[j, pl.ds(first, size), :] = buffer[pl.ds(start + first, size), :]

    def part_of(device, j):
        return pl.multiple_of(lax.rem(device + j, lons) * quarter, quarter)

    def all_of(ref, j, count, send_sem, recv_sem):
        return remote(ref.at[j, pl.ds(0, count)], ref.at[j, pl.ds(0, count)], send_sem, recv_sem, {"lon": ring(1)})

    def spread(j):
        for k in range(1, lons):
            q = ring(k)
            remote(
                s_buf.at[j, pl.ds(part_of(q, j), quarter)], v_buf.at[j, me], p1s.at[j], p1r.at[j], {"lon": q}
            ).start()
        v_buf[j, me] = s_buf[j, pl.ds(part_of(me, j), quarter), :]

    def deliver(j):
        all_of(v_buf, j, lons - 1, p1s.at[j], p1r.at[j]).wait_recv()
        offset = off[j]
        rest = lax.rem(offset, width)
        block = lax.rem(lax.div(offset, width), lons)
        begin = part_of(me, j)
        some = min(32, quarter)
        for first, size in pieces(0, quarter, some):
            place = lax.broadcasted_iota(jnp.int32, (size, levels), 0) + (begin + first)
            turn = jnp.where(place < rest, lax.rem(block + 1, lons), block)
            x = [v_buf[j, s, pl.ds(first, size), :] for s in range(lons)]
            bit = lons // 2
            while bit:
                mask = (turn & bit) != 0
                x = [jnp.where(mask, x[(d - bit) % lons], x[d]) for d in range(lons)]
                bit //= 2
            for d in range(lons):
                g_buf[j, d, pl.ds(PAD + first, size), :] = x[d]
        for d in range(lons):
            g_buf[j, d, :PAD, :] = g_buf[j, (d + 1) % lons, PAD : 2 * PAD, :]
            g_buf[j, d, PAD + quarter :, :] = g_buf[j, (d - 1) % lons, quarter : PAD + quarter, :]
        slot = lax.rem(me + j, lons)

        def give(skip, size):
            there = pl.ds(pl.multiple_of(PAD + begin + skip, PAD), size)
            for k in range(1, lons):
                d = ring(k)
                src = g_buf.at[j, d, pl.ds(skip, size)]
                remote(src, f_buf.at[j, there], p2s.at[j], p2r.at[j], {"lon": d}).start()
            f_buf[j, there, :] = g_buf[j, me, skip : skip + size, :]

        by_slot(slot, lambda: give(0, PAD + quarter), lambda: give(PAD, PAD + quarter), lambda: give(PAD, quarter))

    def by_slot(slot, low_end, high_end, between):
        pl.when(slot == 0)(low_end)
        pl.when(slot == lons - 1)(high_end)
        pl.when((slot > 0) & (slot < lons - 1))(between)

    def count_of(j, size):
        block = f_buf.at[j, pl.ds(0, size)]
        return remote(block, block, p2s.at[j], p2r.at[j], {"lon": ring(1)})

    def arrive(j):
        slot = lax.rem(me + j, lons)
        most = (lons - 1) * quarter
        by_slot(
            slot,
            lambda: count_of(j, most + PAD).wait_recv(),
            lambda: count_of(j, most + PAD).wait_recv(),
            lambda: count_of(j, most + 2 * PAD).wait_recv(),
        )
        east = f_buf[j, PAD : 2 * PAD, :]
        west = f_buf[j, 2 * PAD + width : 3 * PAD + width, :]
        f_buf[j, PAD : 2 * PAD, :] = west
        f_buf[j, 2 * PAD + width : 3 * PAD + width, :] = east
        c = cubic_weights(f_lon[j])
        for first, size in pieces(0, wide, 64):
            r_ext[deep + j, pl.ds(first, size), :] = sum(
                c[m] * f_buf[j, pl.ds(first + PAD - 1 + m, size), :] for m in range(4)
            )
        if j < deep:
            @pl.when(has_low)
            def _():
                low_copy(j).start()
        if j >= rows - deep:
            @pl.when(has_high)
            def _():
                high_copy(j).start()

    def low_copy(j):
        return remote(r_ext.at[deep + j], r_ext.at[deep + rows + j], fs.at[j], fr.at[j], below)

    def high_copy(j):
        m = j - (rows - deep)
        return remote(r_ext.at[deep + j], r_ext.at[m], fs.at[deep + m], fr.at[deep + m], above)

    def settle(j):
        all_of(v_buf, j, lons - 1, p1s.at[j], p1r.at[j]).wait_send()
        slot = lax.rem(me + j, lons)

        def sent(size):
            block = g_buf.at[j, pl.ds(0, lons - 1), pl.ds(0, size)]
            return lambda: remote(block, block, p2s.at[j], p2r.at[j], {"lon": ring(1)}).wait_send()

        by_slot(slot, sent(PAD + quarter), sent(PAD + quarter), sent(quarter))

    ws_refs, vs_refs, zs_refs = (w0, w1, w2), (v0, v1, v2), (z0, z1, z2)
    acc = [jnp.zeros((8, levels), F32) for _ in range(9)]
    lines = 32

    def turn_coefficients():
        tall = jnp.broadcast_to(vc_ref[...], (levels, levels)).T
        place = lax.broadcasted_iota(jnp.int32, (levels, levels), 0)
        column[0] = 2.1 + 2.0 * tall
        column[1] = jnp.where(place < levels - 1, tall, 0.0)
        column[2] = jnp.where(place > 0, tall, 0.0)

    def pack(e):
        matrix = inv_ext[e]
        middle = column[0] + 2.0 * met[e : e + 1, :]
        applied = middle * matrix - column[1] * pltpu.roll(matrix, levels - 1, 0)
        applied = applied - column[2] * pltpu.roll(matrix, 1, 0)
        for n, x in enumerate((matrix, applied)):
            high, low = split(x)
            at = pl.ds(n * levels, levels)
            packed[e, at, :levels] = high
            packed[e, at, levels:] = high
            extra[e, at, :] = low

    def solve(k, e, slot):
        dims = (((1,), (1,)), ((), ()))
        both = lax.dot_general(lhs[slot], packed[e], dims, preferred_element_type=F32)
        both = both + lax.dot_general(lhs[slot, :, :levels], extra[e], dims, preferred_element_type=F32)
        ws_refs[k][e - k, pl.ds(PAD, wide), :] = both[:, :levels]
        if k < e < ext - k - 1:
            zs_refs[k][e - k - 1] = both[:, levels:]

    def load_lhs(slot, first, size, v):
        high, low = split(v)
        lhs[slot, pl.ds(first, size), :levels] = high
        lhs[slot, pl.ds(first, size), levels:] = low

    def begin(e, slot):
        for first, size in pieces(0, wide, lines):
            load_lhs(slot, first, size, r_ext[e, pl.ds(first, size), :])
        solve(0, e, slot)

    def stencil(k, e, first, size):
        w = ws_refs[k]
        n = e - k
        m = met[e : e + 1, :]
        at = pl.ds(first + PAD, size)
        sides = w[n, pl.ds(first + PAD + 1, size), :] + w[n, pl.ds(first + PAD - 1, size), :]
        result = zs_refs[k][n - 1, pl.ds(first, size), :] - (w[n - 1, at, :] + w[n + 1, at, :])
        return result - m * sides

    pairs = {0: ((0, "r", 0), (3, 0, 0)), 1: ((1, "r", 1), (4, 0, 1), (6, 1, 1)),
             2: ((2, "r", 2), (5, 0, 2), (7, 1, 2), (8, 2, 2))}

    def apply(k, e, slot):
        inside = deep <= e < deep + rows
        if k + 1 < ITERS:
            for first, size in pieces(0, wide, lines):
                v = stencil(k, e, first, size)
                load_lhs(slot, first, size, v)
                if inside:
                    vs_refs[k][e - deep, pl.ds(first, size), :] = v
            solve(k + 1, e, slot)
            if inside:
                for first, size in pieces(PAD, PAD + width, lines):
                    gather(k, e, first, size, vs_refs[k][e - deep, pl.ds(first, size), :])
        else:
            for first, size in pieces(PAD, PAD + width, lines):
                v = stencil(k, e, first, size)
                vs_refs[k][e - deep, pl.ds(first, size), :] = v
                gather(k, e, first, size, v)

    def gather(k, e, first, size, v):
        for n, p, q in pairs[k]:
            if p == "r":
                other = r_ext[e, pl.ds(first, size), :]
            elif p == k:
                other = v
            else:
                other = vs_refs[p][e - deep, pl.ds(first, size), :]
            acc[n] = acc[n] + fold(other * v)

    plain = lambda j: 1 <= j <= rows - 3
    edges = [j for j in range(rows) if j < deep or j >= rows - deep]
    order = [j for j in edges if plain(j)] + [j for j in edges if not plain(j)]
    order += [j for j in range(rows) if j not in order]
    outer = sorted(edges, key=lambda j: min(j, rows - 1 - j))
    later = outer + [j for j in range(rows) if j not in outer]
    for copy in fetches:
        copy.wait()
    here = set()

    def need(*wanted):
        for j in first_rows:
            if j in wanted and j not in here:
                here.add(j)
                loads[j].wait()

    waited = False
    for n, j in enumerate(order):
        if not plain(j) and not waited:
            waited = True

            @pl.when(has_low)
            def _():
                up_row.wait_recv()

            @pl.when(has_high)
            def _():
                down_rows.wait_recv()

        need(*range(j - 1, j + 3))
        mix(j)
        if n == 0:
            pl.semaphore_wait(barrier, devices - 1)
        spread(j)
        if n == 0:
            need(0, 1, rows - 1)

            @pl.when(has_high)
            def _():
                up_row.start()

            @pl.when(has_low)
            def _():
                down_rows.start()

            @pl.when(jnp.logical_not(has_low))
            def _():
                clear(t, 0, 1)

            @pl.when(jnp.logical_not(has_high))
            def _():
                clear(t, rows + 1, 2)

        if n == 1:
            for m in range(rows):
                met[deep + m : deep + m + 1, :] = jnp.full((1, levels), metric[m], F32)
            matrices.wait()

            @pl.when(has_high)
            def _():
                up_inv.start()
                for copy in up_met:
                    copy.start()

            @pl.when(has_low)
            def _():
                down_inv.start()
                for copy in down_met:
                    copy.start()

    clear_sides()
    clear_pads()
    turn_coefficients()
    for j in later:
        deliver(j)
    for e in range(deep, deep + rows):
        pack(e)

    @pl.when(has_low)
    def _():
        up_inv.wait_recv()
        for copy in up_met:
            copy.wait_recv()

    @pl.when(has_high)
    def _():
        down_inv.wait_recv()
        for copy in down_met:
            copy.wait_recv()

    for e in list(range(deep)) + list(range(deep + rows, ext)):
        pack(e)

    done = {}
    slots = [0]

    def slot():
        slots[0] += 1
        return slots[0] % 2

    def ready():
        again = True
        while again:
            again = False
            for k in range(ITERS):
                for e in range(k + 1, ext - k - 1):
                    if ("v", k, e) not in done and all(("w", k, e + m) in done for m in (-1, 0, 1)):
                        apply(k, e, slot())
                        done["v", k, e] = True
                        if k + 1 < ITERS:
                            done["w", k + 1, e] = True
                        again = True

    def first_solve(e):
        begin(e, slot())
        done["w", 0, e] = True

    def halo_rows(m):
        @pl.when(has_low)
        def _():
            high_copy(rows - 1 - m).wait_recv()

        @pl.when(has_high)
        def _():
            low_copy(m).wait_recv()

        for e in (deep - 1 - m, deep + rows + m):
            first_solve(e)

    for n, j in enumerate(outer):
        arrive(j)
        first_solve(deep + j)
        if n % 2 == 1 and n >= 3:
            halo_rows(n // 2 - 1)
        ready()
    for j in later[len(outer) :]:
        arrive(j)
        first_solve(deep + j)
        ready()
    halo_rows(deep - 1)
    ready()

    row = jnp.zeros((1, levels), F32)
    for n in range(9):
        row = jnp.where(lane == n, jnp.sum(jnp.sum(acc[n], axis=0, keepdims=True), axis=1, keepdims=True), row)
    part[...] = row
    every[mine] = row

    def tell(peer):
        remote(part, every.at[mine], rs, rr, peer).start()

    if unrolled:
        for peer in others():
            tell(peer)
    else:
        lax.fori_loop(1, devices, lambda k, c: (tell(peer_of(k)), c)[1], 0)
    for j in range(rows):
        where = pl.ds(j, width, stride=rows)
        flat[0][where, :] = r_ext[deep + j, pl.ds(PAD, width), :]
        for k in range(ITERS):
            flat[1 + k][where, :] = vs_refs[k][j, pl.ds(PAD, width), :]
            flat[4 + k][where, :] = ws_refs[k][deep + j - k, pl.ds(2 * PAD, width), :]
    for j in range(rows):
        settle(j)

    @pl.when(has_high)
    def _():
        up_row.wait_send()
        up_inv.wait_send()
        for copy in up_met:
            copy.wait_send()
        for m in range(deep):
            high_copy(rows - deep + m).wait_send()

    @pl.when(has_low)
    def _():
        down_rows.wait_send()
        down_inv.wait_send()
        for copy in down_met:
            copy.wait_send()
        for m in range(deep):
            low_copy(m).wait_send()

    most = every.at[pl.ds(0, devices - 1)]
    totals = remote(most, most, rs, rr, {"lon": ring(1)})
    totals.wait_recv()
    totals.wait_send()
    tot[...] = jnp.broadcast_to(jnp.sum(every[...], axis=0), tot.shape)


def final_kernel(size, tot, r, v0, v1, v2, w0, w1, w2, a_out, p_out, r_out, p_buf, r_buf, a_sem, sem):
    advected = pltpu.make_async_copy(r, a_out, a_sem)
    advected.start()
    total = tot[0:1, :]
    rho, pi = coefficients([jnp.broadcast_to(total[:, n : n + 1], total.shape) for n in range(9)])
    copies = []
    for c in range(r.shape[0] // size):
        at = pl.ds(c * size, size)
        p_buf[at, :] = pi[0] * w0[at, :] + pi[1] * w1[at, :] + pi[2] * w2[at, :]
        r_buf[at, :] = r[at, :] + (rho[0] * v0[at, :] + rho[1] * v1[at, :] + rho[2] * v2[at, :])
        for n, (src, dst) in enumerate(((p_buf, p_out), (r_buf, r_out))):
            copy = pltpu.make_async_copy(src.at[at], dst.at[at], sem.at[n, c])
            copy.start()
            copies.append(copy)
    for copy in copies:
        copy.wait()
    advected.wait()


def body(tracer, offsets, frac_lon, frac_lat, frac_lev, metric, vertical_coef, inverses):
    width, rows, levels = tracer.shape
    lons, lats = lax.axis_size("lon"), lax.axis_size("lat")
    deep = DEEP
    ext, wide, quarter = rows + 2 * deep, width + 2 * PAD, width // lons
    devices = lons * lats
    dma = pltpu.SemaphoreType.DMA
    whole = shape(width * rows, levels)
    field = [pltpu.VMEM((rows, wide, levels), F32)] * 3
    sides = [pltpu.VMEM((ext - 2 * k, wide + 2 * PAD, levels), F32) for k in range(3)]
    verticals = [pltpu.VMEM((ext - 2 * k - 2, wide, levels), F32) for k in range(3)]
    arguments = (offsets, frac_lon, frac_lat, frac_lev, metric, vertical_coef.reshape(1, levels), tracer, inverses)
    arguments = [pltpu.with_memory_space_constraint(x, pltpu.HBM) for x in arguments]
    *flat, tot = pl.pallas_call(
        functools.partial(step_kernel, lons, lats),
        out_shape=[whole] * 7 + [shape(8, levels)],
        in_specs=[HBM] * 8,
        out_specs=[VM] * 8,
        scratch_shapes=[pltpu.VMEM((ext, wide, levels), F32)]
        + field
        + sides
        + verticals
        + [
            pltpu.VMEM((rows + 3, width, levels), F32),
            pltpu.VMEM((2, 2 * width, levels), F32),
            pltpu.VMEM((rows, width, levels), F32),
            pltpu.VMEM((rows, lons, quarter, levels), F32),
            pltpu.VMEM((rows, lons, quarter + 2 * PAD, levels), F32),
            pltpu.VMEM((rows, wide + 2 * PAD, levels), F32),
            pltpu.VMEM((ext, levels, levels), F32),
            pltpu.VMEM((ext, levels), F32),
            pltpu.VMEM((3, levels, levels), F32),
            pltpu.VMEM((ext, 2 * levels, 2 * levels), BF16),
            pltpu.VMEM((ext, 2 * levels, levels), BF16),
            pltpu.VMEM((2, wide, 2 * levels), BF16),
            pltpu.VMEM((1, levels), F32),
            pltpu.VMEM((devices, 1, levels), F32),
            pltpu.SMEM((rows,), jnp.int32),
        ]
        + [pltpu.SMEM((rows,), F32)] * 4
        + [
            pltpu.VMEM((1, levels), F32),
            dma((6,)),
            dma((rows,)),
            dma,
            dma((4,)),
            dma((4,)),
            dma((2 * deep,)),
            dma((2 * deep,)),
        ]
        + [dma((rows,))] * 4
        + [dma((2 * deep,))] * 2
        + [dma] * 2,
        compiler_params=pltpu.CompilerParams(
            collective_id=1, has_side_effects=True, vmem_limit_bytes=40 * 2**20
        ),
    )(*arguments)
    size = min(512, width * rows)
    outs = pl.pallas_call(
        functools.partial(final_kernel, size),
        out_shape=[whole] * 3,
        in_specs=[VM] * 8,
        out_specs=[ANY] * 3,
        scratch_shapes=[pltpu.VMEM((width * rows, levels), F32)] * 2 + [dma, dma((2, width * rows // size))],
        compiler_params=pltpu.CompilerParams(vmem_limit_bytes=16 * 2**20),
    )(tot, *flat)
    return tuple(x.reshape(width, rows, levels) for x in outs)


def solution(mesh):
    cube = P("lon", "lat", None)
    in_specs = (cube, P("lat"), P("lat"), P("lat"), P("lat"), P("lat"), P(), P("lat", None, None))
    return jax.shard_map(
        body, mesh=mesh, in_specs=in_specs, out_specs=(cube, cube, cube), check_vma=False
    )
```

```python
import functools

import jax
import jax.numpy as jnp
from jax import lax
from jax.experimental import pallas as pl
from jax.experimental.pallas import tpu as pltpu
from jax.sharding import PartitionSpec as P

ITERS = 3
DEEP = ITERS
PAD = 8
VM = pl.BlockSpec(memory_space=pltpu.VMEM)
ANY = pl.BlockSpec(memory_space=pl.ANY)
HBM = pl.BlockSpec(memory_space=pltpu.HBM)
F32 = jnp.float32
BF16 = jnp.bfloat16
MESH = pl.DeviceIdType.MESH


def cubic_weights(f):
    return (
        -f * (f - 1.0) * (f - 2.0) * (1.0 / 6.0),
        (f + 1.0) * (f - 1.0) * (f - 2.0) * 0.5,
        -(f + 1.0) * f * (f - 2.0) * 0.5,
        (f + 1.0) * f * (f - 1.0) * (1.0 / 6.0),
    )


def shape(*dims, dtype=F32):
    return jax.ShapeDtypeStruct(dims, dtype)


def signal(sem, peer):
    pl.semaphore_signal(sem, inc=1, device_id=peer, device_id_type=MESH)


def remote(src, dst, send_sem, recv_sem, peer):
    return pltpu.make_async_remote_copy(
        src_ref=src,
        dst_ref=dst,
        send_sem=send_sem,
        recv_sem=recv_sem,
        device_id=peer,
        device_id_type=MESH,
    )


def split(x):
    high = x.astype(BF16)
    return high, (x - high.astype(F32)).astype(BF16)


def pieces(first, last, size):
    out = []
    while first < last:
        step = size if last - first < 2 * size else size
        step = min(step, last - first)
        out.append((first, step))
        first += step
    return out


def fold(x):
    return jnp.sum(x.reshape(x.shape[0] // 8, 8, x.shape[1]), axis=0)


def coefficients(t):
    right = t[:3]
    gram = [[t[3], t[4], t[5]], [t[4], t[6], t[7]], [t[5], t[7], t[8]]]
    zero = jnp.zeros_like(t[0])

    def form(p, q):
        total = zero
        for k in range(3):
            for l in range(3):
                if p[k] is not None and q[l] is not None:
                    total = total + p[k] * q[l] * gram[k][l]
        return total

    def add(p, s, q):
        return [x if y is None else (s * y if x is None else x + s * y) for x, y in zip(p, q)]

    q = [[zero + 1.0, None, None]]
    rho, pi = [None] * 3, [None] * 3
    squares = [form(q[0], q[0])]
    for i in range(ITERS):
        along = form(q[i], rho)
        for k in range(3):
            if q[i][k] is not None:
                along = along + q[i][k] * right[k]
        alpha = along / squares[i]
        pi = add(pi, alpha, q[i])
        rho = add(rho, -alpha, q[i])
        if i + 1 < ITERS:
            z = [zero + 1.0, rho[0], rho[1]]
            new = z
            for l in range(i + 1):
                new = add(new, -form(z, q[l]) / squares[l], q[l])
            q.append(new)
            squares.append(form(new, new))
    return rho, pi


def step_kernel(lons, lats, *refs):
    scalars, (tracer, inv), refs = refs[:6], refs[6:8], refs[8:]
    flat, tot, refs = refs[:7], refs[7], refs[8:]
    (r_ext, v0, v1, v2, w0, w1, w2, z0, z1, z2), refs = refs[:10], refs[10:]
    (t, double, s_buf, v_buf, g_buf, f_buf, inv_ext, met), refs = refs[:8], refs[8:]
    (column, packed, extra, lhs, part, every), refs = refs[:6], refs[6:]
    (off, f_lon, f_lat, f_lev, metric, vc_ref, c_sem), refs = refs[:7], refs[7:]
    (t_sem, i_sem, hs, hr, ns, nr, p1s, p1r, p2s, p2r, fs, fr, rs, rr, word) = refs
    width, rows, levels = tracer.shape
    quarter = width // lons
    deep = DEEP
    ext, wide = rows + 2 * deep, width + 2 * PAD
    me, lat = lax.axis_index("lon"), lax.axis_index("lat")
    ring = lambda k: lax.rem(me + (k + lons), lons)
    has_low, has_high = lat > 0, lat < lats - 1
    below = {"lat": lax.max(lat - 1, 0)}
    above = {"lat": lax.min(lat + 1, lats - 1)}
    devices = lons * lats
    mine = me * lats + lat
    lane = lax.broadcasted_iota(jnp.int32, (1, levels), 1)

    def peer_of(k):
        index = lax.rem(mine + k, devices)
        return {"lon": lax.div(index, lats), "lat": lax.rem(index, lats)}

    first_rows = [0, 1, 2, 3, rows - 1] + list(range(4, rows - 1))
    loads = {j: pltpu.make_async_copy(tracer.at[:, j, :], t.at[j + 1], t_sem.at[j]) for j in range(rows)}
    for j in first_rows:
        loads[j].start()
    fetches = [
        pltpu.make_async_copy(src, dst, c_sem.at[n])
        for n, (src, dst) in enumerate(zip(scalars, (off, f_lon, f_lat, f_lev, metric, vc_ref)))
    ]
    for copy in fetches:
        copy.start()
    matrices = pltpu.make_async_copy(inv, inv_ext.at[pl.ds(deep, rows)], i_sem)
    matrices.start()

    barrier = pltpu.get_barrier_semaphore()
    def others():
        far = lambda n: sorted(range(n), key=lambda k: abs(k - n // 2))
        for b in far(lats):
            for a in far(lons):
                if a or b:
                    yield {"lon": ring(a), "lat": lax.rem(lat + b, lats)}

    unrolled = devices <= 64
    for k in range(1, lons):
        signal(barrier, {"lon": ring(k)})

    @pl.when(has_low)
    def _():
        signal(barrier, below)

    @pl.when(has_high)
    def _():
        signal(barrier, above)

    def pass_along_lat():
        @pl.when(jnp.logical_not(has_high))
        def _():
            signal(word.at[1], below)

        @pl.when(has_low)
        def _():
            pl.semaphore_wait(word.at[0], 1)

        @pl.when(has_high)
        def _():
            signal(word.at[0], above)
            pl.semaphore_wait(word.at[1], 1)

        @pl.when(has_low & has_high)
        def _():
            signal(word.at[1], below)

    def pass_over_lon():
        for k in range(1, lons):
            signal(word.at[2], {"lon": ring(k)})
        pl.semaphore_wait(word.at[2], lons - 1)


    def clear_pads():
        for j in range(rows):
            f_buf[j, :PAD, :] = jnp.zeros((PAD, levels), F32)
            f_buf[j, wide + PAD :, :] = jnp.zeros((PAD, levels), F32)
        for w in (w0, w1, w2):
            for e in range(w.shape[0]):
                w[e, :PAD, :] = jnp.zeros((PAD, levels), F32)
                w[e, wide + PAD :, :] = jnp.zeros((PAD, levels), F32)

    def clear(ref, first, count):
        ref[first : first + count] = jnp.zeros((count,) + ref.shape[1:], F32)

    def clear_sides():
        @pl.when(jnp.logical_not(has_low))
        def _():
            clear(r_ext, 0, deep)
            clear(inv_ext, 0, deep)
            met[:deep, :] = jnp.zeros((deep, levels), F32)

        @pl.when(jnp.logical_not(has_high))
        def _():
            clear(r_ext, deep + rows, deep)
            clear(inv_ext, deep + rows, deep)
            met[deep + rows : ext, :] = jnp.zeros((deep, levels), F32)

    up_row = remote(t.at[rows], t.at[0], hs.at[0], hr.at[0], above)
    down_rows = remote(t.at[pl.ds(1, 2)], t.at[pl.ds(rows + 1, 2)], hs.at[1], hr.at[1], below)
    up_inv = remote(inv_ext.at[pl.ds(rows, deep)], inv_ext.at[pl.ds(0, deep)], hs.at[2], hr.at[2], above)
    down_inv = remote(
        inv_ext.at[pl.ds(deep, deep)], inv_ext.at[pl.ds(deep + rows, deep)], hs.at[3], hr.at[3], below
    )
    up_met = [remote(met.at[rows + m], met.at[m], ns.at[m], nr.at[m], above) for m in range(deep)]
    down_met = [
        remote(met.at[deep + m], met.at[deep + rows + m], ns.at[deep + m], nr.at[deep + m], below)
        for m in range(deep)
    ]
    def mix(j):
        a = cubic_weights(f_lat[j])
        b = cubic_weights(f_lev[j])
        taps = {m: jnp.where((lane + m >= 0) & (lane + m < levels), b[m + 1], 0.0) for m in (-1, 1, 2)}
        buffer = double.at[j % 2]
        for first, size in pieces(0, width, 64):
            at = pl.ds(first, size)
            x = a[0] * t[j, at, :] + a[1] * t[j + 1, at, :] + a[2] * t[j + 2, at, :] + a[3] * t[j + 3, at, :]
            total = b[1] * x
            for m in (-1, 1, 2):
                total = total + taps[m] * pltpu.roll(x, (-m) % levels, 1)
            buffer[at, :] = total
            buffer[pl.ds(width + first, size), :] = total
        start = width - lax.rem(off[j], width)
        for first, size in pieces(0, width, 64):
            s_buf[j, pl.ds(first, size), :] = buffer[pl.ds(start + first, size), :]

    def part_of(device, j):
        return pl.multiple_of(lax.rem(device + j, lons) * quarter, quarter)

    def all_of(ref, j, count, send_sem, recv_sem):
        return remote(ref.at[j, pl.ds(0, count)], ref.at[j, pl.ds(0, count)], send_sem, recv_sem, {"lon": ring(1)})

    def spread(j):
        for k in range(1, lons):
            q = ring(k)
            remote(
                s_buf.at[j, pl.ds(part_of(q, j), quarter)], v_buf.at[j, me], p1s.at[j], p1r.at[j], {"lon": q}
            ).start()
        v_buf[j, me] = s_buf[j, pl.ds(part_of(me, j), quarter), :]

    def deliver(j):
        all_of(v_buf, j, lons - 1, p1s.at[j], p1r.at[j]).wait_recv()
        offset = off[j]
        rest = lax.rem(offset, width)
        block = lax.rem(lax.div(offset, width), lons)
        begin = part_of(me, j)
        some = min(32, quarter)
        for first, size in pieces(0, quarter, some):
            place = lax.broadcasted_iota(jnp.int32, (size, levels), 0) + (begin + first)
            turn = jnp.where(place < rest, lax.rem(block + 1, lons), block)
            x = [v_buf[j, s, pl.ds(first, size), :] for s in range(lons)]
            bit = lons // 2
            while bit:
                mask = (turn & bit) != 0
                x = [jnp.where(mask, x[(d - bit) % lons], x[d]) for d in range(lons)]
                bit //= 2
            for d in range(lons):
                g_buf[j, d, pl.ds(PAD + first, size), :] = x[d]
        for d in range(lons):
            g_buf[j, d, :PAD, :] = g_buf[j, (d + 1) % lons, PAD : 2 * PAD, :]
            g_buf[j, d, PAD + quarter :, :] = g_buf[j, (d - 1) % lons, quarter : PAD + quarter, :]
        slot = lax.rem(me + j, lons)

        def give(skip, size):
            there = pl.ds(pl.multiple_of(PAD + begin + skip, PAD), size)
            for k in range(1, lons):
                d = ring(k)
                src = g_buf.at[j, d, pl.ds(skip, size)]
                remote(src, f_buf.at[j, there], p2s.at[j], p2r.at[j], {"lon": d}).start()
            f_buf[j, there, :] = g_buf[j, me, skip : skip + size, :]

        by_slot(slot, lambda: give(0, PAD + quarter), lambda: give(PAD, PAD + quarter), lambda: give(PAD, quarter))

    def by_slot(slot, low_end, high_end, between):
        pl.when(slot == 0)(low_end)
        pl.when(slot == lons - 1)(high_end)
        pl.when((slot > 0) & (slot < lons - 1))(between)

    def count_of(j, size):
        block = f_buf.at[j, pl.ds(0, size)]
        return remote(block, block, p2s.at[j], p2r.at[j], {"lon": ring(1)})

    def arrive(j):
        slot = lax.rem(me + j, lons)
        most = (lons - 1) * quarter
        by_slot(
            slot,
            lambda: count_of(j, most + PAD).wait_recv(),
            lambda: count_of(j, most + PAD).wait_recv(),
            lambda: count_of(j, most + 2 * PAD).wait_recv(),
        )
        east = f_buf[j, PAD : 2 * PAD, :]
        west = f_buf[j, 2 * PAD + width : 3 * PAD + width, :]
        f_buf[j, PAD : 2 * PAD, :] = west
        f_buf[j, 2 * PAD + width : 3 * PAD + width, :] = east
        c = cubic_weights(f_lon[j])
        for first, size in pieces(0, wide, 64):
            r_ext[deep + j, pl.ds(first, size), :] = sum(
                c[m] * f_buf[j, pl.ds(first + PAD - 1 + m, size), :] for m in range(4)
            )
        if j < deep:
            @pl.when(has_low)
            def _():
                low_copy(j).start()
        if j >= rows - deep:
            @pl.when(has_high)
            def _():
                high_copy(j).start()

    def low_copy(j):
        return remote(r_ext.at[deep + j], r_ext.at[deep + rows + j], fs.at[j], fr.at[j], below)

    def high_copy(j):
        m = j - (rows - deep)
        return remote(r_ext.at[deep + j], r_ext.at[m], fs.at[deep + m], fr.at[deep + m], above)

    def settle(j):
        all_of(v_buf, j, lons - 1, p1s.at[j], p1r.at[j]).wait_send()
        slot = lax.rem(me + j, lons)

        def sent(size):
            block = g_buf.at[j, pl.ds(0, lons - 1), pl.ds(0, size)]
            return lambda: remote(block, block, p2s.at[j], p2r.at[j], {"lon": ring(1)}).wait_send()

        by_slot(slot, sent(PAD + quarter), sent(PAD + quarter), sent(quarter))

    ws_refs, vs_refs, zs_refs = (w0, w1, w2), (v0, v1, v2), (z0, z1, z2)
    acc = [jnp.zeros((8, levels), F32) for _ in range(9)]
    lines = 32

    def turn_coefficients():
        tall = jnp.broadcast_to(vc_ref[...], (levels, levels)).T
        place = lax.broadcasted_iota(jnp.int32, (levels, levels), 0)
        column[0] = 2.1 + 2.0 * tall
        column[1] = jnp.where(place < levels - 1, tall, 0.0)
        column[2] = jnp.where(place > 0, tall, 0.0)

    def pack(e):
        matrix = inv_ext[e]
        middle = column[0] + 2.0 * met[e : e + 1, :]
        applied = middle * matrix - column[1] * pltpu.roll(matrix, levels - 1, 0)
        applied = applied - column[2] * pltpu.roll(matrix, 1, 0)
        for n, x in enumerate((matrix, applied)):
            high, low = split(x)
            at = pl.ds(n * levels, levels)
            packed[e, at, :levels] = high
            packed[e, at, levels:] = high
            extra[e, at, :] = low

    def solve(k, e, slot):
        dims = (((1,), (1,)), ((), ()))
        both = lax.dot_general(lhs[slot], packed[e], dims, preferred_element_type=F32)
        both = both + lax.dot_general(lhs[slot, :, :levels], extra[e], dims, preferred_element_type=F32)
        ws_refs[k][e - k, pl.ds(PAD, wide), :] = both[:, :levels]
        if k < e < ext - k - 1:
            zs_refs[k][e - k - 1] = both[:, levels:]

    def load_lhs(slot, first, size, v):
        high, low = split(v)
        lhs[slot, pl.ds(first, size), :levels] = high
        lhs[slot, pl.ds(first, size), levels:] = low

    def begin(e, slot):
        for first, size in pieces(0, wide, lines):
            load_lhs(slot, first, size, r_ext[e, pl.ds(first, size), :])
        solve(0, e, slot)

    def stencil(k, e, first, size):
        w = ws_refs[k]
        n = e - k
        m = met[e : e + 1, :]
        at = pl.ds(first + PAD, size)
        sides = w[n, pl.ds(first + PAD + 1, size), :] + w[n, pl.ds(first + PAD - 1, size), :]
        result = zs_refs[k][n - 1, pl.ds(first, size), :] - (w[n - 1, at, :] + w[n + 1, at, :])
        return result - m * sides

    pairs = {0: ((0, "r", 0), (3, 0, 0)), 1: ((1, "r", 1), (4, 0, 1), (6, 1, 1)),
             2: ((2, "r", 2), (5, 0, 2), (7, 1, 2), (8, 2, 2))}

    def apply(k, e, slot):
        inside = deep <= e < deep + rows
        if k + 1 < ITERS:
            for first, size in pieces(0, wide, lines):
                v = stencil(k, e, first, size)
                load_lhs(slot, first, size, v)
                if inside:
                    vs_refs[k][e - deep, pl.ds(first, size), :] = v
            solve(k + 1, e, slot)
            if inside:
                for first, size in pieces(PAD, PAD + width, lines):
                    gather(k, e, first, size, vs_refs[k][e - deep, pl.ds(first, size), :])
        else:
            for first, size in pieces(PAD, PAD + width, lines):
                v = stencil(k, e, first, size)
                vs_refs[k][e - deep, pl.ds(first, size), :] = v
                gather(k, e, first, size, v)

    def gather(k, e, first, size, v):
        for n, p, q in pairs[k]:
            if p == "r":
                other = r_ext[e, pl.ds(first, size), :]
            elif p == k:
                other = v
            else:
                other = vs_refs[p][e - deep, pl.ds(first, size), :]
            acc[n] = acc[n] + fold(other * v)

    plain = lambda j: 1 <= j <= rows - 3
    edges = [j for j in range(rows) if j < deep or j >= rows - deep]
    order = [j for j in edges if plain(j)] + [j for j in edges if not plain(j)]
    order += [j for j in range(rows) if j not in order]
    outer = sorted(edges, key=lambda j: min(j, rows - 1 - j))
    later = outer + [j for j in range(rows) if j not in outer]
    for copy in fetches:
        copy.wait()
    here = set()

    def need(*wanted):
        for j in first_rows:
            if j in wanted and j not in here:
                here.add(j)
                loads[j].wait()

    waited = False
    for n, j in enumerate(order):
        if not plain(j) and not waited:
            waited = True

            @pl.when(has_low)
            def _():
                up_row.wait_recv()

            @pl.when(has_high)
            def _():
                down_rows.wait_recv()

        need(*range(j - 1, j + 3))
        mix(j)
        if n == 0:
            pl.semaphore_wait(barrier, (lons - 1) + has_low.astype(jnp.int32) + has_high.astype(jnp.int32))
        spread(j)
        if n == 0:
            need(0, 1, rows - 1)

            @pl.when(has_high)
            def _():
                up_row.start()

            @pl.when(has_low)
            def _():
                down_rows.start()

            @pl.when(jnp.logical_not(has_low))
            def _():
                clear(t, 0, 1)

            @pl.when(jnp.logical_not(has_high))
            def _():
                clear(t, rows + 1, 2)

        if n == 1:
            for m in range(rows):
                met[deep + m : deep + m + 1, :] = jnp.full((1, levels), metric[m], F32)
            matrices.wait()

            @pl.when(has_high)
            def _():
                up_inv.start()
                for copy in up_met:
                    copy.start()

            @pl.when(has_low)
            def _():
                down_inv.start()
                for copy in down_met:
                    copy.start()

    clear_sides()
    clear_pads()
    turn_coefficients()
    pass_along_lat()
    for j in later:
        deliver(j)
    pass_over_lon()
    for e in range(deep, deep + rows):
        pack(e)

    @pl.when(has_low)
    def _():
        up_inv.wait_recv()
        for copy in up_met:
            copy.wait_recv()

    @pl.when(has_high)
    def _():
        down_inv.wait_recv()
        for copy in down_met:
            copy.wait_recv()

    for e in list(range(deep)) + list(range(deep + rows, ext)):
        pack(e)

    done = {}
    slots = [0]

    def slot():
        slots[0] += 1
        return slots[0] % 2

    def ready():
        again = True
        while again:
            again = False
            for k in range(ITERS):
                for e in range(k + 1, ext - k - 1):
                    if ("v", k, e) not in done and all(("w", k, e + m) in done for m in (-1, 0, 1)):
                        apply(k, e, slot())
                        done["v", k, e] = True
                        if k + 1 < ITERS:
                            done["w", k + 1, e] = True
                        again = True

    def first_solve(e):
        begin(e, slot())
        done["w", 0, e] = True

    def halo_rows(m):
        @pl.when(has_low)
        def _():
            high_copy(rows - 1 - m).wait_recv()

        @pl.when(has_high)
        def _():
            low_copy(m).wait_recv()

        for e in (deep - 1 - m, deep + rows + m):
            first_solve(e)

    for n, j in enumerate(outer):
        arrive(j)
        first_solve(deep + j)
        if n % 2 == 1 and n >= 3:
            halo_rows(n // 2 - 1)
        ready()
    for j in later[len(outer) :]:
        arrive(j)
        first_solve(deep + j)
        ready()
    halo_rows(deep - 1)
    ready()

    row = jnp.zeros((1, levels), F32)
    for n in range(9):
        row = jnp.where(lane == n, jnp.sum(jnp.sum(acc[n], axis=0, keepdims=True), axis=1, keepdims=True), row)
    part[...] = row
    every[mine] = row

    def tell(peer):
        remote(part, every.at[mine], rs, rr, peer).start()

    if unrolled:
        for peer in others():
            tell(peer)
    else:
        lax.fori_loop(1, devices, lambda k, c: (tell(peer_of(k)), c)[1], 0)
    for j in range(rows):
        where = pl.ds(j, width, stride=rows)
        flat[0][where, :] = r_ext[deep + j, pl.ds(PAD, width), :]
        for k in range(ITERS):
            flat[1 + k][where, :] = vs_refs[k][j, pl.ds(PAD, width), :]
            flat[4 + k][where, :] = ws_refs[k][deep + j - k, pl.ds(2 * PAD, width), :]
    for j in range(rows):
        settle(j)

    @pl.when(has_high)
    def _():
        up_row.wait_send()
        up_inv.wait_send()
        for copy in up_met:
            copy.wait_send()
        for m in range(deep):
            high_copy(rows - deep + m).wait_send()

    @pl.when(has_low)
    def _():
        down_rows.wait_send()
        down_inv.wait_send()
        for copy in down_met:
            copy.wait_send()
        for m in range(deep):
            low_copy(m).wait_send()

    most = every.at[pl.ds(0, devices - 1)]
    totals = remote(most, most, rs, rr, {"lon": ring(1)})
    totals.wait_recv()
    totals.wait_send()
    tot[...] = jnp.broadcast_to(jnp.sum(every[...], axis=0), tot.shape)


def final_kernel(size, tot, r, v0, v1, v2, w0, w1, w2, a_out, p_out, r_out, p_buf, r_buf, a_sem, sem):
    advected = pltpu.make_async_copy(r, a_out, a_sem)
    advected.start()
    total = tot[0:1, :]
    rho, pi = coefficients([jnp.broadcast_to(total[:, n : n + 1], total.shape) for n in range(9)])
    copies = []
    for c in range(r.shape[0] // size):
        at = pl.ds(c * size, size)
        p_buf[at, :] = pi[0] * w0[at, :] + pi[1] * w1[at, :] + pi[2] * w2[at, :]
        r_buf[at, :] = r[at, :] + (rho[0] * v0[at, :] + rho[1] * v1[at, :] + rho[2] * v2[at, :])
        for n, (src, dst) in enumerate(((p_buf, p_out), (r_buf, r_out))):
            copy = pltpu.make_async_copy(src.at[at], dst.at[at], sem.at[n, c])
            copy.start()
            copies.append(copy)
    for copy in copies:
        copy.wait()
    advected.wait()


def body(tracer, offsets, frac_lon, frac_lat, frac_lev, metric, vertical_coef, inverses):
    width, rows, levels = tracer.shape
    lons, lats = lax.axis_size("lon"), lax.axis_size("lat")
    deep = DEEP
    ext, wide, quarter = rows + 2 * deep, width + 2 * PAD, width // lons
    devices = lons * lats
    dma = pltpu.SemaphoreType.DMA
    whole = shape(width * rows, levels)
    field = [pltpu.VMEM((rows, wide, levels), F32)] * 3
    sides = [pltpu.VMEM((ext - 2 * k, wide + 2 * PAD, levels), F32) for k in range(3)]
    verticals = [pltpu.VMEM((ext - 2 * k - 2, wide, levels), F32) for k in range(3)]
    arguments = (offsets, frac_lon, frac_lat, frac_lev, metric, vertical_coef.reshape(1, levels), tracer, inverses)
    arguments = [pltpu.with_memory_space_constraint(x, pltpu.HBM) for x in arguments]
    *flat, tot = pl.pallas_call(
        functools.partial(step_kernel, lons, lats),
        out_shape=[whole] * 7 + [shape(8, levels)],
        in_specs=[HBM] * 8,
        out_specs=[VM] * 8,
        scratch_shapes=[pltpu.VMEM((ext, wide, levels), F32)]
        + field
        + sides
        + verticals
        + [
            pltpu.VMEM((rows + 3, width, levels), F32),
            pltpu.VMEM((2, 2 * width, levels), F32),
            pltpu.VMEM((rows, width, levels), F32),
            pltpu.VMEM((rows, lons, quarter, levels), F32),
            pltpu.VMEM((rows, lons, quarter + 2 * PAD, levels), F32),
            pltpu.VMEM((rows, wide + 2 * PAD, levels), F32),
            pltpu.VMEM((ext, levels, levels), F32),
            pltpu.VMEM((ext, levels), F32),
            pltpu.VMEM((3, levels, levels), F32),
            pltpu.VMEM((ext, 2 * levels, 2 * levels), BF16),
            pltpu.VMEM((ext, 2 * levels, levels), BF16),
            pltpu.VMEM((2, wide, 2 * levels), BF16),
            pltpu.VMEM((1, levels), F32),
            pltpu.VMEM((devices, 1, levels), F32),
            pltpu.SMEM((rows,), jnp.int32),
        ]
        + [pltpu.SMEM((rows,), F32)] * 4
        + [
            pltpu.VMEM((1, levels), F32),
            dma((6,)),
            dma((rows,)),
            dma,
            dma((4,)),
            dma((4,)),
            dma((2 * deep,)),
            dma((2 * deep,)),
        ]
        + [dma((rows,))] * 4
        + [dma((2 * deep,))] * 2
        + [dma] * 2
        + [pltpu.SemaphoreType.REGULAR((3,))],
        compiler_params=pltpu.CompilerParams(
            collective_id=1, has_side_effects=True, vmem_limit_bytes=40 * 2**20
        ),
    )(*arguments)
    size = min(512, width * rows)
    outs = pl.pallas_call(
        functools.partial(final_kernel, size),
        out_shape=[whole] * 3,
        in_specs=[VM] * 8,
        out_specs=[ANY] * 3,
        scratch_shapes=[pltpu.VMEM((width * rows, levels), F32)] * 2 + [dma, dma((2, width * rows // size))],
        compiler_params=pltpu.CompilerParams(vmem_limit_bytes=16 * 2**20),
    )(tot, *flat)
    return tuple(x.reshape(width, rows, levels) for x in outs)


def solution(mesh):
    cube = P("lon", "lat", None)
    in_specs = (cube, P("lat"), P("lat"), P("lat"), P("lat"), P("lat"), P(), P("lat", None, None))
    return jax.shard_map(
        body, mesh=mesh, in_specs=in_specs, out_specs=(cube, cube, cube), check_vma=False
    )
```

```python
import functools

import jax
import jax.numpy as jnp
from jax import lax
from jax.experimental import pallas as pl
from jax.experimental.pallas import tpu as pltpu
from jax.sharding import PartitionSpec as P

ITERS = 3
DEEP = ITERS
PAD = 8
VM = pl.BlockSpec(memory_space=pltpu.VMEM)
ANY = pl.BlockSpec(memory_space=pl.ANY)
HBM = pl.BlockSpec(memory_space=pltpu.HBM)
F32 = jnp.float32
BF16 = jnp.bfloat16
MESH = pl.DeviceIdType.MESH


def cubic_weights(f):
    return (
        -f * (f - 1.0) * (f - 2.0) * (1.0 / 6.0),
        (f + 1.0) * (f - 1.0) * (f - 2.0) * 0.5,
        -(f + 1.0) * f * (f - 2.0) * 0.5,
        (f + 1.0) * f * (f - 1.0) * (1.0 / 6.0),
    )


def shape(*dims, dtype=F32):
    return jax.ShapeDtypeStruct(dims, dtype)


def signal(sem, peer):
    pl.semaphore_signal(sem, inc=1, device_id=peer, device_id_type=MESH)


def remote(src, dst, send_sem, recv_sem, peer):
    return pltpu.make_async_remote_copy(
        src_ref=src,
        dst_ref=dst,
        send_sem=send_sem,
        recv_sem=recv_sem,
        device_id=peer,
        device_id_type=MESH,
    )


def split(x):
    high = x.astype(BF16)
    return high, (x - high.astype(F32)).astype(BF16)


def pieces(first, last, size):
    out = []
    while first < last:
        step = size if last - first < 2 * size else size
        step = min(step, last - first)
        out.append((first, step))
        first += step
    return out


def fold(x):
    return jnp.sum(x.reshape(x.shape[0] // 8, 8, x.shape[1]), axis=0)


def coefficients(t):
    right = t[:3]
    gram = [[t[3], t[4], t[5]], [t[4], t[6], t[7]], [t[5], t[7], t[8]]]
    zero = jnp.zeros_like(t[0])

    def form(p, q):
        total = zero
        for k in range(3):
            for l in range(3):
                if p[k] is not None and q[l] is not None:
                    total = total + p[k] * q[l] * gram[k][l]
        return total

    def add(p, s, q):
        return [x if y is None else (s * y if x is None else x + s * y) for x, y in zip(p, q)]

    q = [[zero + 1.0, None, None]]
    rho, pi = [None] * 3, [None] * 3
    squares = [form(q[0], q[0])]
    for i in range(ITERS):
        along = form(q[i], rho)
        for k in range(3):
            if q[i][k] is not None:
                along = along + q[i][k] * right[k]
        alpha = along / squares[i]
        pi = add(pi, alpha, q[i])
        rho = add(rho, -alpha, q[i])
        if i + 1 < ITERS:
            z = [zero + 1.0, rho[0], rho[1]]
            new = z
            for l in range(i + 1):
                new = add(new, -form(z, q[l]) / squares[l], q[l])
            q.append(new)
            squares.append(form(new, new))
    return rho, pi


def step_kernel(lons, lats, *refs):
    scalars, (tracer, inv), refs = refs[:6], refs[6:8], refs[8:]
    flat, tot, refs = refs[:7], refs[7], refs[8:]
    (r_ext, v0, v1, v2, w0, w1, w2, z0, z1, z2), refs = refs[:10], refs[10:]
    (t, double, s_buf, v_buf, g_buf, f_buf, inv_ext, met), refs = refs[:8], refs[8:]
    (column, packed, extra, packed_far, extra_far, lhs, part, every), refs = refs[:8], refs[8:]
    (off, f_lon, f_lat, f_lev, metric, vc_ref, c_sem), refs = refs[:7], refs[7:]
    (t_sem, i_sem, hs, hr, ns, nr, p1s, p1r, p2s, p2r, fs, fr, rs, rr, word) = refs
    width, rows, levels = tracer.shape
    quarter = width // lons
    deep = DEEP
    ext, wide = rows + 2 * deep, width + 2 * PAD
    me, lat = lax.axis_index("lon"), lax.axis_index("lat")
    ring = lambda k: lax.rem(me + (k + lons), lons)
    has_low, has_high = lat > 0, lat < lats - 1
    below = {"lat": lax.max(lat - 1, 0)}
    above = {"lat": lax.min(lat + 1, lats - 1)}
    devices = lons * lats
    mine = me * lats + lat
    lane = lax.broadcasted_iota(jnp.int32, (1, levels), 1)

    def peer_of(k):
        index = lax.rem(mine + k, devices)
        return {"lon": lax.div(index, lats), "lat": lax.rem(index, lats)}

    first_rows = [0, 1, 2, 3, rows - 1] + list(range(4, rows - 1))
    loads = {j: pltpu.make_async_copy(tracer.at[:, j, :], t.at[j + 1], t_sem.at[j]) for j in range(rows)}
    for j in first_rows:
        loads[j].start()
    fetches = [
        pltpu.make_async_copy(src, dst, c_sem.at[n])
        for n, (src, dst) in enumerate(zip(scalars, (off, f_lon, f_lat, f_lev, metric, vc_ref)))
    ]
    for copy in fetches:
        copy.start()
    matrices = pltpu.make_async_copy(inv, inv_ext.at[pl.ds(deep, rows)], i_sem)
    matrices.start()

    barrier = pltpu.get_barrier_semaphore()
    unrolled = devices <= 64
    for k in range(1, lons):
        signal(barrier, {"lon": ring(k)})

    @pl.when(has_low)
    def _():
        signal(barrier, below)

    @pl.when(has_high)
    def _():
        signal(barrier, above)

    def pass_along_lat():
        @pl.when(jnp.logical_not(has_high))
        def _():
            signal(word.at[1], below)

        @pl.when(has_low)
        def _():
            pl.semaphore_wait(word.at[0], 1)

        @pl.when(has_high)
        def _():
            signal(word.at[0], above)
            pl.semaphore_wait(word.at[1], 1)

        @pl.when(has_low & has_high)
        def _():
            signal(word.at[1], below)

    def pass_over_lon():
        for k in range(1, lons):
            signal(word.at[2], {"lon": ring(k)})
        pl.semaphore_wait(word.at[2], lons - 1)


    def clear_pads():
        for j in range(rows):
            f_buf[j, :PAD, :] = jnp.zeros((PAD, levels), F32)
            f_buf[j, wide + PAD :, :] = jnp.zeros((PAD, levels), F32)
        for w in (w0, w1, w2):
            for e in range(w.shape[0]):
                w[e, :PAD, :] = jnp.zeros((PAD, levels), F32)
                w[e, wide + PAD :, :] = jnp.zeros((PAD, levels), F32)

    def clear(ref, first, count):
        ref[first : first + count] = jnp.zeros((count,) + ref.shape[1:], F32)

    def clear_sides():
        @pl.when(jnp.logical_not(has_low))
        def _():
            clear(r_ext, 0, deep)
            clear(inv_ext, 0, deep)
            met[:deep, :] = jnp.zeros((deep, levels), F32)

        @pl.when(jnp.logical_not(has_high))
        def _():
            clear(r_ext, deep + rows, deep)
            clear(inv_ext, deep + rows, deep)
            met[deep + rows : ext, :] = jnp.zeros((deep, levels), F32)

    up_row = remote(t.at[rows], t.at[0], hs.at[0], hr.at[0], above)
    down_rows = remote(t.at[pl.ds(1, 2)], t.at[pl.ds(rows + 1, 2)], hs.at[1], hr.at[1], below)
    up_inv = remote(inv_ext.at[pl.ds(rows, deep)], inv_ext.at[pl.ds(0, deep)], hs.at[2], hr.at[2], above)
    down_inv = remote(
        inv_ext.at[pl.ds(deep, deep)], inv_ext.at[pl.ds(deep + rows, deep)], hs.at[3], hr.at[3], below
    )
    up_met = [remote(met.at[rows + m], met.at[m], ns.at[m], nr.at[m], above) for m in range(deep)]
    down_met = [
        remote(met.at[deep + m], met.at[deep + rows + m], ns.at[deep + m], nr.at[deep + m], below)
        for m in range(deep)
    ]
    def mix(j):
        a = cubic_weights(f_lat[j])
        b = cubic_weights(f_lev[j])
        taps = {m: jnp.where((lane + m >= 0) & (lane + m < levels), b[m + 1], 0.0) for m in (-1, 1, 2)}
        buffer = double.at[j % 2]
        for first, size in pieces(0, width, 64):
            at = pl.ds(first, size)
            x = a[0] * t[j, at, :] + a[1] * t[j + 1, at, :] + a[2] * t[j + 2, at, :] + a[3] * t[j + 3, at, :]
            total = b[1] * x
            for m in (-1, 1, 2):
                total = total + taps[m] * pltpu.roll(x, (-m) % levels, 1)
            buffer[at, :] = total
            buffer[pl.ds(width + first, size), :] = total
        start = width - lax.rem(off[j], width)
        for first, size in pieces(0, width, 64):
            s_buf[j, pl.ds(first, size), :] = buffer[pl.ds(start + first, size), :]

    def part_of(device, j):
        return pl.multiple_of(lax.rem(device + j, lons) * quarter, quarter)

    def all_of(ref, j, count, send_sem, recv_sem):
        return remote(ref.at[j, pl.ds(0, count)], ref.at[j, pl.ds(0, count)], send_sem, recv_sem, {"lon": ring(1)})

    def spread(j):
        for k in range(1, lons):
            q = ring(k)
            remote(
                s_buf.at[j, pl.ds(part_of(q, j), quarter)], v_buf.at[j, me], p1s.at[j], p1r.at[j], {"lon": q}
            ).start()
        v_buf[j, me] = s_buf[j, pl.ds(part_of(me, j), quarter), :]

    def deliver(j):
        all_of(v_buf, j, lons - 1, p1s.at[j], p1r.at[j]).wait_recv()
        offset = off[j]
        rest = lax.rem(offset, width)
        block = lax.rem(lax.div(offset, width), lons)
        begin = part_of(me, j)
        some = min(32, quarter)
        for first, size in pieces(0, quarter, some):
            place = lax.broadcasted_iota(jnp.int32, (size, levels), 0) + (begin + first)
            turn = jnp.where(place < rest, lax.rem(block + 1, lons), block)
            x = [v_buf[j, s, pl.ds(first, size), :] for s in range(lons)]
            bit = lons // 2
            while bit:
                mask = (turn & bit) != 0
                x = [jnp.where(mask, x[(d - bit) % lons], x[d]) for d in range(lons)]
                bit //= 2
            for d in range(lons):
                g_buf[j, d, pl.ds(PAD + first, size), :] = x[d]
        for d in range(lons):
            g_buf[j, d, :PAD, :] = g_buf[j, (d + 1) % lons, PAD : 2 * PAD, :]
            g_buf[j, d, PAD + quarter :, :] = g_buf[j, (d - 1) % lons, quarter : PAD + quarter, :]
        slot = lax.rem(me + j, lons)

        def give(skip, size):
            there = pl.ds(pl.multiple_of(PAD + begin + skip, PAD), size)
            for k in range(1, lons):
                d = ring(k)
                src = g_buf.at[j, d, pl.ds(skip, size)]
                remote(src, f_buf.at[j, there], p2s.at[j], p2r.at[j], {"lon": d}).start()
            f_buf[j, there, :] = g_buf[j, me, skip : skip + size, :]

        by_slot(slot, lambda: give(0, PAD + quarter), lambda: give(PAD, PAD + quarter), lambda: give(PAD, quarter))

    def by_slot(slot, low_end, high_end, between):
        pl.when(slot == 0)(low_end)
        pl.when(slot == lons - 1)(high_end)
        pl.when((slot > 0) & (slot < lons - 1))(between)

    def count_of(j, size):
        block = f_buf.at[j, pl.ds(0, size)]
        return remote(block, block, p2s.at[j], p2r.at[j], {"lon": ring(1)})

    def arrive(j):
        slot = lax.rem(me + j, lons)
        most = (lons - 1) * quarter
        by_slot(
            slot,
            lambda: count_of(j, most + PAD).wait_recv(),
            lambda: count_of(j, most + PAD).wait_recv(),
            lambda: count_of(j, most + 2 * PAD).wait_recv(),
        )
        east = f_buf[j, PAD : 2 * PAD, :]
        west = f_buf[j, 2 * PAD + width : 3 * PAD + width, :]
        f_buf[j, PAD : 2 * PAD, :] = west
        f_buf[j, 2 * PAD + width : 3 * PAD + width, :] = east
        c = cubic_weights(f_lon[j])
        for first, size in pieces(0, wide, 64):
            r_ext[deep + j, pl.ds(first, size), :] = sum(
                c[m] * f_buf[j, pl.ds(first + PAD - 1 + m, size), :] for m in range(4)
            )
        if j < deep:
            @pl.when(has_low)
            def _():
                low_copy(j).start()
        if j >= rows - deep:
            @pl.when(has_high)
            def _():
                high_copy(j).start()

    def low_copy(j):
        return remote(r_ext.at[deep + j], r_ext.at[deep + rows + j], fs.at[j], fr.at[j], below)

    def high_copy(j):
        m = j - (rows - deep)
        return remote(r_ext.at[deep + j], r_ext.at[m], fs.at[deep + m], fr.at[deep + m], above)

    def settle(j):
        all_of(v_buf, j, lons - 1, p1s.at[j], p1r.at[j]).wait_send()
        slot = lax.rem(me + j, lons)

        def sent(size):
            block = g_buf.at[j, pl.ds(0, lons - 1), pl.ds(0, size)]
            return lambda: remote(block, block, p2s.at[j], p2r.at[j], {"lon": ring(1)}).wait_send()

        by_slot(slot, sent(PAD + quarter), sent(PAD + quarter), sent(quarter))

    ws_refs, vs_refs, zs_refs = (w0, w1, w2), (v0, v1, v2), (z0, z1, z2)
    acc = [jnp.zeros((8, levels), F32) for _ in range(9)]
    lines = 32

    def turn_coefficients():
        tall = jnp.broadcast_to(vc_ref[...], (levels, levels)).T
        place = lax.broadcasted_iota(jnp.int32, (levels, levels), 0)
        column[0] = 2.1 + 2.0 * tall
        column[1] = jnp.where(place < levels - 1, tall, 0.0)
        column[2] = jnp.where(place > 0, tall, 0.0)

    def pack(e):
        matrix = inv_ext[e]
        middle = column[0] + 2.0 * met[e : e + 1, :]
        applied = middle * matrix - column[1] * pltpu.roll(matrix, levels - 1, 0)
        applied = applied - column[2] * pltpu.roll(matrix, 1, 0)
        for n, x in enumerate((matrix, applied)):
            high, low = split(x)
            at = pl.ds(n * levels, levels)
            packed[e, at, :levels] = high
            packed[e, at, levels:] = high
            extra[e, at, :] = low

    def pack_far(side, near):
        product = inv_ext[near[0]]
        for e in near[1:]:
            product = jnp.dot(product, inv_ext[e], precision=lax.Precision.HIGHEST, preferred_element_type=F32)
        high, low = split(product)
        packed_far[side, :, :levels] = high
        packed_far[side, :, levels:] = high
        extra_far[side] = low

    def far_row(side, e, inner, slot):
        dims = (((1,), (1,)), ((), ()))
        for first, size in pieces(0, wide, lines):
            load_lhs(slot, first, size, r_ext[e, pl.ds(first, size), :])
        change = lax.dot_general(lhs[slot], packed_far[side], dims, preferred_element_type=F32)
        change = change + lax.dot_general(
            lhs[slot, :, :levels], extra_far[side], dims, preferred_element_type=F32
        )
        sign = 1.0 if deep % 2 else -1.0
        for first, size in pieces(PAD, PAD + width, lines):
            at = pl.ds(first, size)
            v = v2[inner - deep, at, :] - sign * change[first : first + size]
            v2[inner - deep, at, :] = v
            gather(ITERS - 1, inner, first, size, v)

    def solve(k, e, slot):
        dims = (((1,), (1,)), ((), ()))
        both = lax.dot_general(lhs[slot], packed[e], dims, preferred_element_type=F32)
        both = both + lax.dot_general(lhs[slot, :, :levels], extra[e], dims, preferred_element_type=F32)
        ws_refs[k][e - k, pl.ds(PAD, wide), :] = both[:, :levels]
        if k < e < ext - k - 1:
            zs_refs[k][e - k - 1] = both[:, levels:]

    def load_lhs(slot, first, size, v):
        high, low = split(v)
        lhs[slot, pl.ds(first, size), :levels] = high
        lhs[slot, pl.ds(first, size), levels:] = low

    def begin(e, slot):
        for first, size in pieces(0, wide, lines):
            load_lhs(slot, first, size, r_ext[e, pl.ds(first, size), :])
        solve(0, e, slot)

    def stencil(k, e, first, size):
        w = ws_refs[k]
        n = e - k
        m = met[e : e + 1, :]
        at = pl.ds(first + PAD, size)
        sides = w[n, pl.ds(first + PAD + 1, size), :] + w[n, pl.ds(first + PAD - 1, size), :]
        result = zs_refs[k][n - 1, pl.ds(first, size), :] - (w[n - 1, at, :] + w[n + 1, at, :])
        return result - m * sides

    pairs = {0: ((0, "r", 0), (3, 0, 0)), 1: ((1, "r", 1), (4, 0, 1), (6, 1, 1)),
             2: ((2, "r", 2), (5, 0, 2), (7, 1, 2), (8, 2, 2))}

    def apply(k, e, slot):
        inside = deep <= e < deep + rows
        if k + 1 < ITERS:
            for first, size in pieces(0, wide, lines):
                v = stencil(k, e, first, size)
                load_lhs(slot, first, size, v)
                if inside:
                    vs_refs[k][e - deep, pl.ds(first, size), :] = v
            solve(k + 1, e, slot)
            if inside:
                for first, size in pieces(PAD, PAD + width, lines):
                    gather(k, e, first, size, vs_refs[k][e - deep, pl.ds(first, size), :])
        else:
            for first, size in pieces(PAD, PAD + width, lines):
                v = stencil(k, e, first, size)
                vs_refs[k][e - deep, pl.ds(first, size), :] = v
                if deep < e < deep + rows - 1:
                    gather(k, e, first, size, v)

    def gather(k, e, first, size, v):
        for n, p, q in pairs[k]:
            if p == "r":
                other = r_ext[e, pl.ds(first, size), :]
            elif p == k:
                other = v
            else:
                other = vs_refs[p][e - deep, pl.ds(first, size), :]
            acc[n] = acc[n] + fold(other * v)

    plain = lambda j: 1 <= j <= rows - 3
    edges = [j for j in range(rows) if j < deep or j >= rows - deep]
    inner = [j for j in range(rows) if j not in edges]
    reach = [j for j in edges if j == 0] + [j for j in reversed(edges) if j > rows - 3]
    order = [j for j in edges if plain(j)] + reach[:1] + inner[:1] + reach[1:] + inner[1:]
    outer = sorted(edges, key=lambda j: min(j, rows - 1 - j))
    later = outer + [j for j in range(rows) if j not in outer]
    for copy in fetches:
        copy.wait()
    here = set()

    def need(*wanted):
        for j in first_rows:
            if j in wanted and j not in here:
                here.add(j)
                loads[j].wait()

    low_here = high_here = False
    for n, j in enumerate(order):
        if j == 0 and not low_here:
            low_here = True
            pl.when(has_low)(lambda: up_row.wait_recv())
        if j > rows - 3 and not high_here:
            high_here = True
            pl.when(has_high)(lambda: down_rows.wait_recv())
        need(*range(j - 1, j + 3))
        mix(j)
        if n == 0:
            pl.semaphore_wait(barrier, (lons - 1) + has_low.astype(jnp.int32) + has_high.astype(jnp.int32))
        spread(j)
        if n == 0:
            need(0, 1, rows - 1)

            @pl.when(has_high)
            def _():
                up_row.start()

            @pl.when(has_low)
            def _():
                down_rows.start()

            @pl.when(jnp.logical_not(has_low))
            def _():
                clear(t, 0, 1)

            @pl.when(jnp.logical_not(has_high))
            def _():
                clear(t, rows + 1, 2)

        if n == 1:
            for m in range(rows):
                met[deep + m : deep + m + 1, :] = jnp.full((1, levels), metric[m], F32)
            matrices.wait()

            @pl.when(has_high)
            def _():
                up_inv.start()
                for copy in up_met:
                    copy.start()

            @pl.when(has_low)
            def _():
                down_inv.start()
                for copy in down_met:
                    copy.start()

    clear_sides()
    clear_pads()
    turn_coefficients()
    pass_along_lat()
    for j in later:
        deliver(j)
    pass_over_lon()
    for e in range(deep, deep + rows):
        pack(e)

    @pl.when(has_low)
    def _():
        up_inv.wait_recv()
        for copy in up_met:
            copy.wait_recv()

    @pl.when(has_high)
    def _():
        down_inv.wait_recv()
        for copy in down_met:
            copy.wait_recv()

    for e in list(range(1, deep)) + list(range(deep + rows, ext - 1)):
        pack(e)
    pack_far(0, range(deep - 1, -1, -1))
    pack_far(1, range(deep + rows, ext))
    clear(w0, 0, 1)
    clear(w0, ext - 1, 1)

    done = {}
    slots = [0]

    def slot():
        slots[0] += 1
        return slots[0] % 2

    def ready():
        again = True
        while again:
            again = False
            for k in range(ITERS):
                for e in range(k + 1, ext - k - 1):
                    if ("v", k, e) not in done and all(("w", k, e + m) in done for m in (-1, 0, 1)):
                        apply(k, e, slot())
                        done["v", k, e] = True
                        if k + 1 < ITERS:
                            done["w", k + 1, e] = True
                        again = True

    def first_solve(e):
        begin(e, slot())
        done["w", 0, e] = True

    def halo_rows(m):
        @pl.when(has_low)
        def _():
            high_copy(rows - 1 - m).wait_recv()

        @pl.when(has_high)
        def _():
            low_copy(m).wait_recv()

        for side, e in enumerate((deep - 1 - m, deep + rows + m)):
            if m < deep - 1:
                first_solve(e)
            else:
                far_row(side, e, (deep, deep + rows - 1)[side], slot())

    done["w", 0, 0] = done["w", 0, ext - 1] = True
    for n, j in enumerate(outer):
        arrive(j)
        first_solve(deep + j)
        if n % 2 == 1 and n >= 3:
            halo_rows(n // 2 - 1)
        ready()
    for j in later[len(outer) :]:
        arrive(j)
        first_solve(deep + j)
        ready()
    halo_rows(deep - 1)

    row = jnp.zeros((1, levels), F32)
    for n in range(9):
        row = jnp.where(lane == n, jnp.sum(jnp.sum(acc[n], axis=0, keepdims=True), axis=1, keepdims=True), row)
    part[...] = row
    every[mine] = row

    def tell(peer):
        remote(part, every.at[mine], rs, rr, peer).start()

    if unrolled:
        for n in range(lats):
            row_of = jnp.where(lat >= lats // 2, n, lats - 1 - n)
            for a in range(1, lons):
                tell({"lon": ring(a), "lat": row_of})

            @pl.when(row_of != lat)
            def _():
                tell({"lat": row_of})
    else:
        lax.fori_loop(1, devices, lambda k, c: (tell(peer_of(k)), c)[1], 0)
    for j in range(rows):
        where = pl.ds(j, width, stride=rows)
        flat[0][where, :] = r_ext[deep + j, pl.ds(PAD, width), :]
        for k in range(ITERS):
            flat[1 + k][where, :] = vs_refs[k][j, pl.ds(PAD, width), :]
            flat[4 + k][where, :] = ws_refs[k][deep + j - k, pl.ds(2 * PAD, width), :]
    for j in range(rows):
        settle(j)

    @pl.when(has_high)
    def _():
        up_row.wait_send()
        up_inv.wait_send()
        for copy in up_met:
            copy.wait_send()
        for m in range(deep):
            high_copy(rows - deep + m).wait_send()

    @pl.when(has_low)
    def _():
        down_rows.wait_send()
        down_inv.wait_send()
        for copy in down_met:
            copy.wait_send()
        for m in range(deep):
            low_copy(m).wait_send()

    most = every.at[pl.ds(0, devices - 1)]
    totals = remote(most, most, rs, rr, {"lon": ring(1)})
    totals.wait_recv()
    totals.wait_send()
    tot[...] = jnp.broadcast_to(jnp.sum(every[...], axis=0), tot.shape)


def final_kernel(size, tot, r, v0, v1, v2, w0, w1, w2, a_out, p_out, r_out, p_buf, r_buf, a_sem, sem):
    advected = pltpu.make_async_copy(r, a_out, a_sem)
    advected.start()
    total = tot[0:1, :]
    rho, pi = coefficients([jnp.broadcast_to(total[:, n : n + 1], total.shape) for n in range(9)])
    copies = []
    for c in range(r.shape[0] // size):
        at = pl.ds(c * size, size)
        p_buf[at, :] = pi[0] * w0[at, :] + pi[1] * w1[at, :] + pi[2] * w2[at, :]
        r_buf[at, :] = r[at, :] + (rho[0] * v0[at, :] + rho[1] * v1[at, :] + rho[2] * v2[at, :])
        for n, (src, dst) in enumerate(((p_buf, p_out), (r_buf, r_out))):
            copy = pltpu.make_async_copy(src.at[at], dst.at[at], sem.at[n, c])
            copy.start()
            copies.append(copy)
    for copy in copies:
        copy.wait()
    advected.wait()


def body(tracer, offsets, frac_lon, frac_lat, frac_lev, metric, vertical_coef, inverses):
    width, rows, levels = tracer.shape
    lons, lats = lax.axis_size("lon"), lax.axis_size("lat")
    deep = DEEP
    ext, wide, quarter = rows + 2 * deep, width + 2 * PAD, width // lons
    devices = lons * lats
    dma = pltpu.SemaphoreType.DMA
    whole = shape(width * rows, levels)
    field = [pltpu.VMEM((rows, wide, levels), F32)] * 3
    sides = [pltpu.VMEM((ext - 2 * k, wide + 2 * PAD, levels), F32) for k in range(3)]
    verticals = [pltpu.VMEM((ext - 2 * k - 2, wide, levels), F32) for k in range(3)]
    arguments = (offsets, frac_lon, frac_lat, frac_lev, metric, vertical_coef.reshape(1, levels), tracer, inverses)
    arguments = [pltpu.with_memory_space_constraint(x, pltpu.HBM) for x in arguments]
    *flat, tot = pl.pallas_call(
        functools.partial(step_kernel, lons, lats),
        out_shape=[whole] * 7 + [shape(8, levels)],
        in_specs=[HBM] * 8,
        out_specs=[VM] * 8,
        scratch_shapes=[pltpu.VMEM((ext, wide, levels), F32)]
        + field
        + sides
        + verticals
        + [
            pltpu.VMEM((rows + 3, width, levels), F32),
            pltpu.VMEM((2, 2 * width, levels), F32),
            pltpu.VMEM((rows, width, levels), F32),
            pltpu.VMEM((rows, lons, quarter, levels), F32),
            pltpu.VMEM((rows, lons, quarter + 2 * PAD, levels), F32),
            pltpu.VMEM((rows, wide + 2 * PAD, levels), F32),
            pltpu.VMEM((ext, levels, levels), F32),
            pltpu.VMEM((ext, levels), F32),
            pltpu.VMEM((3, levels, levels), F32),
            pltpu.VMEM((ext, 2 * levels, 2 * levels), BF16),
            pltpu.VMEM((ext, 2 * levels, levels), BF16),
            pltpu.VMEM((2, levels, 2 * levels), BF16),
            pltpu.VMEM((2, levels, levels), BF16),
            pltpu.VMEM((2, wide, 2 * levels), BF16),
            pltpu.VMEM((1, levels), F32),
            pltpu.VMEM((devices, 1, levels), F32),
            pltpu.SMEM((rows,), jnp.int32),
        ]
        + [pltpu.SMEM((rows,), F32)] * 4
        + [
            pltpu.VMEM((1, levels), F32),
            dma((6,)),
            dma((rows,)),
            dma,
            dma((4,)),
            dma((4,)),
            dma((2 * deep,)),
            dma((2 * deep,)),
        ]
        + [dma((rows,))] * 4
        + [dma((2 * deep,))] * 2
        + [dma] * 2
        + [pltpu.SemaphoreType.REGULAR((3,))],
        compiler_params=pltpu.CompilerParams(
            collective_id=1, has_side_effects=True, vmem_limit_bytes=40 * 2**20
        ),
    )(*arguments)
    size = min(512, width * rows)
    outs = pl.pallas_call(
        functools.partial(final_kernel, size),
        out_shape=[whole] * 3,
        in_specs=[VM] * 8,
        out_specs=[ANY] * 3,
        scratch_shapes=[pltpu.VMEM((width * rows, levels), F32)] * 2 + [dma, dma((2, width * rows // size))],
        compiler_params=pltpu.CompilerParams(vmem_limit_bytes=16 * 2**20),
    )(tot, *flat)
    return tuple(x.reshape(width, rows, levels) for x in outs)


def solution(mesh):
    cube = P("lon", "lat", None)
    in_specs = (cube, P("lat"), P("lat"), P("lat"), P("lat"), P("lat"), P(), P("lat", None, None))
    return jax.shard_map(
        body, mesh=mesh, in_specs=in_specs, out_specs=(cube, cube, cube), check_vma=False
    )
```

```python
import functools

import jax
import jax.numpy as jnp
from jax import lax
from jax.experimental import pallas as pl
from jax.experimental.pallas import tpu as pltpu
from jax.sharding import PartitionSpec as P

ITERS = 3
DEEP = ITERS
PAD = 8
VM = pl.BlockSpec(memory_space=pltpu.VMEM)
ANY = pl.BlockSpec(memory_space=pl.ANY)
HBM = pl.BlockSpec(memory_space=pltpu.HBM)
F32 = jnp.float32
BF16 = jnp.bfloat16
MESH = pl.DeviceIdType.MESH


def cubic_weights(f):
    return (
        -f * (f - 1.0) * (f - 2.0) * (1.0 / 6.0),
        (f + 1.0) * (f - 1.0) * (f - 2.0) * 0.5,
        -(f + 1.0) * f * (f - 2.0) * 0.5,
        (f + 1.0) * f * (f - 1.0) * (1.0 / 6.0),
    )


def shape(*dims, dtype=F32):
    return jax.ShapeDtypeStruct(dims, dtype)


def signal(sem, peer):
    pl.semaphore_signal(sem, inc=1, device_id=peer, device_id_type=MESH)


def remote(src, dst, send_sem, recv_sem, peer):
    return pltpu.make_async_remote_copy(
        src_ref=src,
        dst_ref=dst,
        send_sem=send_sem,
        recv_sem=recv_sem,
        device_id=peer,
        device_id_type=MESH,
    )


def split(x):
    high = x.astype(BF16)
    return high, (x - high.astype(F32)).astype(BF16)


def pieces(first, last, size):
    out = []
    while first < last:
        step = size if last - first < 2 * size else size
        step = min(step, last - first)
        out.append((first, step))
        first += step
    return out


def fold(x):
    return jnp.sum(x.reshape(x.shape[0] // 8, 8, x.shape[1]), axis=0)


def coefficients(t):
    right = t[:3]
    gram = [[t[3], t[4], t[5]], [t[4], t[6], t[7]], [t[5], t[7], t[8]]]
    zero = jnp.zeros_like(t[0])

    def form(p, q):
        total = zero
        for k in range(3):
            for l in range(3):
                if p[k] is not None and q[l] is not None:
                    total = total + p[k] * q[l] * gram[k][l]
        return total

    def add(p, s, q):
        return [x if y is None else (s * y if x is None else x + s * y) for x, y in zip(p, q)]

    q = [[zero + 1.0, None, None]]
    rho, pi = [None] * 3, [None] * 3
    squares = [form(q[0], q[0])]
    for i in range(ITERS):
        along = form(q[i], rho)
        for k in range(3):
            if q[i][k] is not None:
                along = along + q[i][k] * right[k]
        alpha = along / squares[i]
        pi = add(pi, alpha, q[i])
        rho = add(rho, -alpha, q[i])
        if i + 1 < ITERS:
            z = [zero + 1.0, rho[0], rho[1]]
            new = z
            for l in range(i + 1):
                new = add(new, -form(z, q[l]) / squares[l], q[l])
            q.append(new)
            squares.append(form(new, new))
    return rho, pi


def step_kernel(lons, lats, *refs):
    scalars, (tracer, inv), refs = refs[:6], refs[6:8], refs[8:]
    flat, tot, refs = refs[:7], refs[7], refs[8:]
    (r_ext, v0, v1, v2, w0, w1, w2, z0, z1, z2), refs = refs[:10], refs[10:]
    (t, double, s_buf, v_buf, g_buf, f_buf, inv_ext, met), refs = refs[:8], refs[8:]
    (column, packed, extra, packed_far, extra_far, lhs, part, every), refs = refs[:8], refs[8:]
    (off, f_lon, f_lat, f_lev, metric, vc_ref, c_sem), refs = refs[:7], refs[7:]
    (t_sem, i_sem, hs, hr, ns, nr, p1s, p1r, p2s, p2r, fs, fr, rs, rr, word) = refs
    width, rows, levels = tracer.shape
    quarter = width // lons
    deep = DEEP
    ext, wide = rows + 2 * deep, width + 2 * PAD
    me, lat = lax.axis_index("lon"), lax.axis_index("lat")
    ring = lambda k: lax.rem(me + (k + lons), lons)
    turns = sorted(range(1, lons), key=lambda k: (k + 1) % 2)
    has_low, has_high = lat > 0, lat < lats - 1
    below = {"lat": lax.max(lat - 1, 0)}
    above = {"lat": lax.min(lat + 1, lats - 1)}
    devices = lons * lats
    mine = me * lats + lat
    lane = lax.broadcasted_iota(jnp.int32, (1, levels), 1)

    def peer_of(k):
        index = lax.rem(mine + k, devices)
        return {"lon": lax.div(index, lats), "lat": lax.rem(index, lats)}

    first_rows = [0, 1, 2, 3, rows - 1] + list(range(4, rows - 1))
    loads = {j: pltpu.make_async_copy(tracer.at[:, j, :], t.at[j + 1], t_sem.at[j]) for j in range(rows)}
    for j in first_rows:
        loads[j].start()
    fetches = [
        pltpu.make_async_copy(src, dst, c_sem.at[n])
        for n, (src, dst) in enumerate(zip(scalars, (off, f_lon, f_lat, f_lev, metric, vc_ref)))
    ]
    for copy in fetches:
        copy.start()
    matrices = pltpu.make_async_copy(inv, inv_ext.at[pl.ds(deep, rows)], i_sem)
    matrices.start()

    barrier = pltpu.get_barrier_semaphore()
    unrolled = devices <= 64
    for k in range(1, lons):
        signal(barrier, {"lon": ring(k)})

    @pl.when(has_low)
    def _():
        signal(barrier, below)

    @pl.when(has_high)
    def _():
        signal(barrier, above)

    def pass_along_lat():
        @pl.when(jnp.logical_not(has_high))
        def _():
            signal(word.at[1], below)

        @pl.when(has_low)
        def _():
            pl.semaphore_wait(word.at[0], 1)

        @pl.when(has_high)
        def _():
            signal(word.at[0], above)
            pl.semaphore_wait(word.at[1], 1)

        @pl.when(has_low & has_high)
        def _():
            signal(word.at[1], below)

    def pass_over_lon():
        for k in range(1, lons):
            signal(word.at[2], {"lon": ring(k)})
        pl.semaphore_wait(word.at[2], lons - 1)


    def clear_pads():
        for j in range(rows):
            f_buf[j, :PAD, :] = jnp.zeros((PAD, levels), F32)
            f_buf[j, wide + PAD :, :] = jnp.zeros((PAD, levels), F32)
        for w in (w0, w1, w2):
            for e in range(w.shape[0]):
                w[e, :PAD, :] = jnp.zeros((PAD, levels), F32)
                w[e, wide + PAD :, :] = jnp.zeros((PAD, levels), F32)

    def clear(ref, first, count):
        ref[first : first + count] = jnp.zeros((count,) + ref.shape[1:], F32)

    def clear_sides():
        @pl.when(jnp.logical_not(has_low))
        def _():
            clear(r_ext, 0, deep)
            clear(inv_ext, 0, deep)
            met[:deep, :] = jnp.zeros((deep, levels), F32)

        @pl.when(jnp.logical_not(has_high))
        def _():
            clear(r_ext, deep + rows, deep)
            clear(inv_ext, deep + rows, deep)
            met[deep + rows : ext, :] = jnp.zeros((deep, levels), F32)

    up_row = remote(t.at[rows], t.at[0], hs.at[0], hr.at[0], above)
    down_rows = remote(t.at[pl.ds(1, 2)], t.at[pl.ds(rows + 1, 2)], hs.at[1], hr.at[1], below)
    up_inv = remote(inv_ext.at[pl.ds(rows, deep)], inv_ext.at[pl.ds(0, deep)], hs.at[2], hr.at[2], above)
    down_inv = remote(
        inv_ext.at[pl.ds(deep, deep)], inv_ext.at[pl.ds(deep + rows, deep)], hs.at[3], hr.at[3], below
    )
    up_met = [remote(met.at[rows + m], met.at[m], ns.at[m], nr.at[m], above) for m in range(deep)]
    down_met = [
        remote(met.at[deep + m], met.at[deep + rows + m], ns.at[deep + m], nr.at[deep + m], below)
        for m in range(deep)
    ]
    def mix(j):
        a = cubic_weights(f_lat[j])
        b = cubic_weights(f_lev[j])
        taps = {m: jnp.where((lane + m >= 0) & (lane + m < levels), b[m + 1], 0.0) for m in (-1, 1, 2)}
        buffer = double.at[j % 2]
        for first, size in pieces(0, width, 64):
            at = pl.ds(first, size)
            x = a[0] * t[j, at, :] + a[1] * t[j + 1, at, :] + a[2] * t[j + 2, at, :] + a[3] * t[j + 3, at, :]
            total = b[1] * x
            for m in (-1, 1, 2):
                total = total + taps[m] * pltpu.roll(x, (-m) % levels, 1)
            buffer[at, :] = total
            buffer[pl.ds(width + first, size), :] = total
        start = width - lax.rem(off[j], width)
        for first, size in pieces(0, width, 64):
            s_buf[j, pl.ds(first, size), :] = buffer[pl.ds(start + first, size), :]

    def part_of(device, j):
        return pl.multiple_of(lax.rem(device + j, lons) * quarter, quarter)

    def all_of(ref, j, count, send_sem, recv_sem):
        return remote(ref.at[j, pl.ds(0, count)], ref.at[j, pl.ds(0, count)], send_sem, recv_sem, {"lon": ring(1)})

    def spread(j):
        for k in turns:
            q = ring(k)
            remote(
                s_buf.at[j, pl.ds(part_of(q, j), quarter)], v_buf.at[j, me], p1s.at[j], p1r.at[j], {"lon": q}
            ).start()
        v_buf[j, me] = s_buf[j, pl.ds(part_of(me, j), quarter), :]

    def deliver(j):
        all_of(v_buf, j, lons - 1, p1s.at[j], p1r.at[j]).wait_recv()
        offset = off[j]
        rest = lax.rem(offset, width)
        block = lax.rem(lax.div(offset, width), lons)
        begin = part_of(me, j)
        some = min(32, quarter)
        for first, size in pieces(0, quarter, some):
            place = lax.broadcasted_iota(jnp.int32, (size, levels), 0) + (begin + first)
            turn = jnp.where(place < rest, lax.rem(block + 1, lons), block)
            x = [v_buf[j, s, pl.ds(first, size), :] for s in range(lons)]
            bit = lons // 2
            while bit:
                mask = (turn & bit) != 0
                x = [jnp.where(mask, x[(d - bit) % lons], x[d]) for d in range(lons)]
                bit //= 2
            for d in range(lons):
                g_buf[j, d, pl.ds(PAD + first, size), :] = x[d]
        for d in range(lons):
            g_buf[j, d, :PAD, :] = g_buf[j, (d + 1) % lons, PAD : 2 * PAD, :]
            g_buf[j, d, PAD + quarter :, :] = g_buf[j, (d - 1) % lons, quarter : PAD + quarter, :]
        slot = lax.rem(me + j, lons)

        def give(skip, size):
            there = pl.ds(pl.multiple_of(PAD + begin + skip, PAD), size)
            for k in turns:
                d = ring(k)
                src = g_buf.at[j, d, pl.ds(skip, size)]
                remote(src, f_buf.at[j, there], p2s.at[j], p2r.at[j], {"lon": d}).start()
            f_buf[j, there, :] = g_buf[j, me, skip : skip + size, :]

        by_slot(slot, lambda: give(0, PAD + quarter), lambda: give(PAD, PAD + quarter), lambda: give(PAD, quarter))

    def by_slot(slot, low_end, high_end, between):
        pl.when(slot == 0)(low_end)
        pl.when(slot == lons - 1)(high_end)
        pl.when((slot > 0) & (slot < lons - 1))(between)

    def count_of(j, size):
        block = f_buf.at[j, pl.ds(0, size)]
        return remote(block, block, p2s.at[j], p2r.at[j], {"lon": ring(1)})

    def arrive(j):
        slot = lax.rem(me + j, lons)
        most = (lons - 1) * quarter
        by_slot(
            slot,
            lambda: count_of(j, most + PAD).wait_recv(),
            lambda: count_of(j, most + PAD).wait_recv(),
            lambda: count_of(j, most + 2 * PAD).wait_recv(),
        )
        east = f_buf[j, PAD : 2 * PAD, :]
        west = f_buf[j, 2 * PAD + width : 3 * PAD + width, :]
        f_buf[j, PAD : 2 * PAD, :] = west
        f_buf[j, 2 * PAD + width : 3 * PAD + width, :] = east
        c = cubic_weights(f_lon[j])
        for first, size in pieces(0, wide, 64):
            r_ext[deep + j, pl.ds(first, size), :] = sum(
                c[m] * f_buf[j, pl.ds(first + PAD - 1 + m, size), :] for m in range(4)
            )
        if j < deep:
            @pl.when(has_low)
            def _():
                low_copy(j).start()
        if j >= rows - deep:
            @pl.when(has_high)
            def _():
                high_copy(j).start()

    def low_copy(j):
        return remote(r_ext.at[deep + j], r_ext.at[deep + rows + j], fs.at[j], fr.at[j], below)

    def high_copy(j):
        m = j - (rows - deep)
        return remote(r_ext.at[deep + j], r_ext.at[m], fs.at[deep + m], fr.at[deep + m], above)

    def settle(j):
        all_of(v_buf, j, lons - 1, p1s.at[j], p1r.at[j]).wait_send()
        slot = lax.rem(me + j, lons)

        def sent(size):
            block = g_buf.at[j, pl.ds(0, lons - 1), pl.ds(0, size)]
            return lambda: remote(block, block, p2s.at[j], p2r.at[j], {"lon": ring(1)}).wait_send()

        by_slot(slot, sent(PAD + quarter), sent(PAD + quarter), sent(quarter))

    ws_refs, vs_refs, zs_refs = (w0, w1, w2), (v0, v1, v2), (z0, z1, z2)
    acc = [jnp.zeros((8, levels), F32) for _ in range(9)]
    lines = 32

    def turn_coefficients():
        tall = jnp.broadcast_to(vc_ref[...], (levels, levels)).T
        place = lax.broadcasted_iota(jnp.int32, (levels, levels), 0)
        column[0] = 2.1 + 2.0 * tall
        column[1] = jnp.where(place < levels - 1, tall, 0.0)
        column[2] = jnp.where(place > 0, tall, 0.0)

    def pack(e):
        matrix = inv_ext[e]
        middle = column[0] + 2.0 * met[e : e + 1, :]
        applied = middle * matrix - column[1] * pltpu.roll(matrix, levels - 1, 0)
        applied = applied - column[2] * pltpu.roll(matrix, 1, 0)
        for n, x in enumerate((matrix, applied)):
            high, low = split(x)
            at = pl.ds(n * levels, levels)
            packed[e, at, :levels] = high
            packed[e, at, levels:] = high
            extra[e, at, :] = low

    def pack_far(side, near):
        product = inv_ext[near[0]]
        for e in near[1:]:
            product = jnp.dot(product, inv_ext[e], precision=lax.Precision.HIGHEST, preferred_element_type=F32)
        high, low = split(product)
        packed_far[side, :, :levels] = high
        packed_far[side, :, levels:] = high
        extra_far[side] = low

    def far_row(side, e, inner, slot):
        dims = (((1,), (1,)), ((), ()))
        for first, size in pieces(0, wide, lines):
            load_lhs(slot, first, size, r_ext[e, pl.ds(first, size), :])
        change = lax.dot_general(lhs[slot], packed_far[side], dims, preferred_element_type=F32)
        change = change + lax.dot_general(
            lhs[slot, :, :levels], extra_far[side], dims, preferred_element_type=F32
        )
        sign = 1.0 if deep % 2 else -1.0
        for first, size in pieces(PAD, PAD + width, lines):
            at = pl.ds(first, size)
            v = v2[inner - deep, at, :] - sign * change[first : first + size]
            v2[inner - deep, at, :] = v
            gather(ITERS - 1, inner, first, size, v)

    def solve(k, e, slot):
        dims = (((1,), (1,)), ((), ()))
        both = lax.dot_general(lhs[slot], packed[e], dims, preferred_element_type=F32)
        both = both + lax.dot_general(lhs[slot, :, :levels], extra[e], dims, preferred_element_type=F32)
        ws_refs[k][e - k, pl.ds(PAD, wide), :] = both[:, :levels]
        if k < e < ext - k - 1:
            zs_refs[k][e - k - 1] = both[:, levels:]

    def load_lhs(slot, first, size, v):
        high, low = split(v)
        lhs[slot, pl.ds(first, size), :levels] = high
        lhs[slot, pl.ds(first, size), levels:] = low

    def begin(e, slot):
        for first, size in pieces(0, wide, lines):
            load_lhs(slot, first, size, r_ext[e, pl.ds(first, size), :])
        solve(0, e, slot)

    def stencil(k, e, first, size):
        w = ws_refs[k]
        n = e - k
        m = met[e : e + 1, :]
        at = pl.ds(first + PAD, size)
        sides = w[n, pl.ds(first + PAD + 1, size), :] + w[n, pl.ds(first + PAD - 1, size), :]
        result = zs_refs[k][n - 1, pl.ds(first, size), :] - (w[n - 1, at, :] + w[n + 1, at, :])
        return result - m * sides

    pairs = {0: ((0, "r", 0), (3, 0, 0)), 1: ((1, "r", 1), (4, 0, 1), (6, 1, 1)),
             2: ((2, "r", 2), (5, 0, 2), (7, 1, 2), (8, 2, 2))}

    def apply(k, e, slot):
        inside = deep <= e < deep + rows
        if k + 1 < ITERS:
            for first, size in pieces(0, wide, lines):
                v = stencil(k, e, first, size)
                load_lhs(slot, first, size, v)
                if inside:
                    vs_refs[k][e - deep, pl.ds(first, size), :] = v
            solve(k + 1, e, slot)
            if inside:
                for first, size in pieces(PAD, PAD + width, lines):
                    gather(k, e, first, size, vs_refs[k][e - deep, pl.ds(first, size), :])
        else:
            for first, size in pieces(PAD, PAD + width, lines):
                v = stencil(k, e, first, size)
                vs_refs[k][e - deep, pl.ds(first, size), :] = v
                if deep < e < deep + rows - 1:
                    gather(k, e, first, size, v)

    def gather(k, e, first, size, v):
        for n, p, q in pairs[k]:
            if p == "r":
                other = r_ext[e, pl.ds(first, size), :]
            elif p == k:
                other = v
            else:
                other = vs_refs[p][e - deep, pl.ds(first, size), :]
            acc[n] = acc[n] + fold(other * v)

    plain = lambda j: 1 <= j <= rows - 3
    edges = [j for j in range(rows) if j < deep or j >= rows - deep]
    inner = [j for j in range(rows) if j not in edges]
    reach = [j for j in edges if j == 0] + [j for j in reversed(edges) if j > rows - 3]
    order = [j for j in edges if plain(j)] + reach[:1] + inner[:1] + reach[1:] + inner[1:]
    outer = sorted(edges, key=lambda j: min(j, rows - 1 - j))
    later = outer + [j for j in range(rows) if j not in outer]
    for copy in fetches:
        copy.wait()
    here = set()

    def need(*wanted):
        for j in first_rows:
            if j in wanted and j not in here:
                here.add(j)
                loads[j].wait()

    low_here = high_here = False
    for n, j in enumerate(order):
        if j == 0 and not low_here:
            low_here = True
            pl.when(has_low)(lambda: up_row.wait_recv())
        if j > rows - 3 and not high_here:
            high_here = True
            pl.when(has_high)(lambda: down_rows.wait_recv())
        need(*range(j - 1, j + 3))
        mix(j)
        if n == 0:
            pl.semaphore_wait(barrier, (lons - 1) + has_low.astype(jnp.int32) + has_high.astype(jnp.int32))
        spread(j)
        if n == 0:
            need(0, 1, rows - 1)

            @pl.when(has_high)
            def _():
                up_row.start()

            @pl.when(has_low)
            def _():
                down_rows.start()

            @pl.when(jnp.logical_not(has_low))
            def _():
                clear(t, 0, 1)

            @pl.when(jnp.logical_not(has_high))
            def _():
                clear(t, rows + 1, 2)

        if n == 1:
            for m in range(rows):
                met[deep + m : deep + m + 1, :] = jnp.full((1, levels), metric[m], F32)
            matrices.wait()

            @pl.when(has_high)
            def _():
                up_inv.start()
                for copy in up_met:
                    copy.start()

            @pl.when(has_low)
            def _():
                down_inv.start()
                for copy in down_met:
                    copy.start()

    clear_sides()
    clear_pads()
    turn_coefficients()
    pass_along_lat()
    for j in later:
        deliver(j)
    pass_over_lon()
    for e in range(deep, deep + rows):
        pack(e)

    @pl.when(has_low)
    def _():
        up_inv.wait_recv()
        for copy in up_met:
            copy.wait_recv()

    @pl.when(has_high)
    def _():
        down_inv.wait_recv()
        for copy in down_met:
            copy.wait_recv()

    for e in list(range(1, deep)) + list(range(deep + rows, ext - 1)):
        pack(e)
    pack_far(0, range(deep - 1, -1, -1))
    pack_far(1, range(deep + rows, ext))
    clear(w0, 0, 1)
    clear(w0, ext - 1, 1)

    done = {}
    slots = [0]

    def slot():
        slots[0] += 1
        return slots[0] % 2

    def ready():
        again = True
        while again:
            again = False
            for k in range(ITERS):
                for e in range(k + 1, ext - k - 1):
                    if ("v", k, e) not in done and all(("w", k, e + m) in done for m in (-1, 0, 1)):
                        apply(k, e, slot())
                        done["v", k, e] = True
                        if k + 1 < ITERS:
                            done["w", k + 1, e] = True
                        again = True

    def first_solve(e):
        begin(e, slot())
        done["w", 0, e] = True

    def halo_rows(m):
        @pl.when(has_low)
        def _():
            high_copy(rows - 1 - m).wait_recv()

        @pl.when(has_high)
        def _():
            low_copy(m).wait_recv()

        for side, e in enumerate((deep - 1 - m, deep + rows + m)):
            if m < deep - 1:
                first_solve(e)
            else:
                far_row(side, e, (deep, deep + rows - 1)[side], slot())

    done["w", 0, 0] = done["w", 0, ext - 1] = True
    for n, j in enumerate(outer):
        arrive(j)
        first_solve(deep + j)
        if n % 2 == 1 and n >= 3:
            halo_rows(n // 2 - 1)
        ready()
    for j in later[len(outer) :]:
        arrive(j)
        first_solve(deep + j)
        ready()
    halo_rows(deep - 1)

    row = jnp.zeros((1, levels), F32)
    for n in range(9):
        row = jnp.where(lane == n, jnp.sum(jnp.sum(acc[n], axis=0, keepdims=True), axis=1, keepdims=True), row)
    part[...] = row
    every[mine] = row

    def tell(peer):
        remote(part, every.at[mine], rs, rr, peer).start()

    if unrolled:
        for n in range(lats):
            row_of = jnp.where(lat >= lats // 2, n, lats - 1 - n)
            for a in range(1, lons):
                tell({"lon": ring(a), "lat": row_of})

            @pl.when(row_of != lat)
            def _():
                tell({"lat": row_of})
    else:
        lax.fori_loop(1, devices, lambda k, c: (tell(peer_of(k)), c)[1], 0)
    for j in range(rows):
        where = pl.ds(j, width, stride=rows)
        flat[0][where, :] = r_ext[deep + j, pl.ds(PAD, width), :]
        for k in range(ITERS):
            flat[1 + k][where, :] = vs_refs[k][j, pl.ds(PAD, width), :]
            flat[4 + k][where, :] = ws_refs[k][deep + j - k, pl.ds(2 * PAD, width), :]
    for j in range(rows):
        settle(j)

    @pl.when(has_high)
    def _():
        up_row.wait_send()
        up_inv.wait_send()
        for copy in up_met:
            copy.wait_send()
        for m in range(deep):
            high_copy(rows - deep + m).wait_send()

    @pl.when(has_low)
    def _():
        down_rows.wait_send()
        down_inv.wait_send()
        for copy in down_met:
            copy.wait_send()
        for m in range(deep):
            low_copy(m).wait_send()

    most = every.at[pl.ds(0, devices - 1)]
    totals = remote(most, most, rs, rr, {"lon": ring(1)})
    totals.wait_recv()
    totals.wait_send()
    tot[...] = jnp.broadcast_to(jnp.sum(every[...], axis=0), tot.shape)


def final_kernel(size, tot, r, v0, v1, v2, w0, w1, w2, a_out, p_out, r_out, p_buf, r_buf, a_sem, sem):
    advected = pltpu.make_async_copy(r, a_out, a_sem)
    advected.start()
    total = tot[0:1, :]
    rho, pi = coefficients([jnp.broadcast_to(total[:, n : n + 1], total.shape) for n in range(9)])
    copies = []
    for c in range(r.shape[0] // size):
        at = pl.ds(c * size, size)
        p_buf[at, :] = pi[0] * w0[at, :] + pi[1] * w1[at, :] + pi[2] * w2[at, :]
        r_buf[at, :] = r[at, :] + (rho[0] * v0[at, :] + rho[1] * v1[at, :] + rho[2] * v2[at, :])
        for n, (src, dst) in enumerate(((p_buf, p_out), (r_buf, r_out))):
            copy = pltpu.make_async_copy(src.at[at], dst.at[at], sem.at[n, c])
            copy.start()
            copies.append(copy)
    for copy in copies:
        copy.wait()
    advected.wait()


def body(tracer, offsets, frac_lon, frac_lat, frac_lev, metric, vertical_coef, inverses):
    width, rows, levels = tracer.shape
    lons, lats = lax.axis_size("lon"), lax.axis_size("lat")
    deep = DEEP
    ext, wide, quarter = rows + 2 * deep, width + 2 * PAD, width // lons
    devices = lons * lats
    dma = pltpu.SemaphoreType.DMA
    whole = shape(width * rows, levels)
    field = [pltpu.VMEM((rows, wide, levels), F32)] * 3
    sides = [pltpu.VMEM((ext - 2 * k, wide + 2 * PAD, levels), F32) for k in range(3)]
    verticals = [pltpu.VMEM((ext - 2 * k - 2, wide, levels), F32) for k in range(3)]
    arguments = (offsets, frac_lon, frac_lat, frac_lev, metric, vertical_coef.reshape(1, levels), tracer, inverses)
    arguments = [pltpu.with_memory_space_constraint(x, pltpu.HBM) for x in arguments]
    *flat, tot = pl.pallas_call(
        functools.partial(step_kernel, lons, lats),
        out_shape=[whole] * 7 + [shape(8, levels)],
        in_specs=[HBM] * 8,
        out_specs=[VM] * 8,
        scratch_shapes=[pltpu.VMEM((ext, wide, levels), F32)]
        + field
        + sides
        + verticals
        + [
            pltpu.VMEM((rows + 3, width, levels), F32),
            pltpu.VMEM((2, 2 * width, levels), F32),
            pltpu.VMEM((rows, width, levels), F32),
            pltpu.VMEM((rows, lons, quarter, levels), F32),
            pltpu.VMEM((rows, lons, quarter + 2 * PAD, levels), F32),
            pltpu.VMEM((rows, wide + 2 * PAD, levels), F32),
            pltpu.VMEM((ext, levels, levels), F32),
            pltpu.VMEM((ext, levels), F32),
            pltpu.VMEM((3, levels, levels), F32),
            pltpu.VMEM((ext, 2 * levels, 2 * levels), BF16),
            pltpu.VMEM((ext, 2 * levels, levels), BF16),
            pltpu.VMEM((2, levels, 2 * levels), BF16),
            pltpu.VMEM((2, levels, levels), BF16),
            pltpu.VMEM((2, wide, 2 * levels), BF16),
            pltpu.VMEM((1, levels), F32),
            pltpu.VMEM((devices, 1, levels), F32),
            pltpu.SMEM((rows,), jnp.int32),
        ]
        + [pltpu.SMEM((rows,), F32)] * 4
        + [
            pltpu.VMEM((1, levels), F32),
            dma((6,)),
            dma((rows,)),
            dma,
            dma((4,)),
            dma((4,)),
            dma((2 * deep,)),
            dma((2 * deep,)),
        ]
        + [dma((rows,))] * 4
        + [dma((2 * deep,))] * 2
        + [dma] * 2
        + [pltpu.SemaphoreType.REGULAR((3,))],
        compiler_params=pltpu.CompilerParams(
            collective_id=1, has_side_effects=True, vmem_limit_bytes=40 * 2**20
        ),
    )(*arguments)
    size = min(512, width * rows)
    outs = pl.pallas_call(
        functools.partial(final_kernel, size),
        out_shape=[whole] * 3,
        in_specs=[VM] * 8,
        out_specs=[ANY] * 3,
        scratch_shapes=[pltpu.VMEM((width * rows, levels), F32)] * 2 + [dma, dma((2, width * rows // size))],
        compiler_params=pltpu.CompilerParams(vmem_limit_bytes=16 * 2**20),
    )(tot, *flat)
    return tuple(x.reshape(width, rows, levels) for x in outs)


def solution(mesh):
    cube = P("lon", "lat", None)
    in_specs = (cube, P("lat"), P("lat"), P("lat"), P("lat"), P("lat"), P(), P("lat", None, None))
    return jax.shard_map(
        body, mesh=mesh, in_specs=in_specs, out_specs=(cube, cube, cube), check_vma=False
    )
```
